32 devices in a mesh: data: 4 (over y, z), group: 8 (over x, core).
Axes of the slice: x: 4, y: 2, z: 2, core: 2. Of those that a mesh axis runs over, the one named last changes fastest.
The devices are a block of a 4x4x8 slice.
Arguments:
- latents: bfloat16 [4096, 384], P(('data', 'group')), parts along dimension 0
- hint_embed: bfloat16 [4096, 384], P(('data', 'group')), parts along dimension 0
- in_qkv: bfloat16 [2, 17, 384, 1152], replicated
- in_proj: bfloat16 [2, 17, 6, 64, 384], replicated
- in_up: bfloat16 [2, 17, 384, 1536], replicated
- in_down: bfloat16 [2, 17, 1536, 384], replicated
- in_norm: bfloat16 [2, 17, 4, 384], replicated
- out_qkv: bfloat16 [16, 384, 1152], replicated
- out_proj: bfloat16 [16, 6, 64, 384], replicated
- out_up: bfloat16 [16, 384, 1536], replicated
- out_down: bfloat16 [16, 1536, 384], replicated
- out_norm: bfloat16 [16, 4, 384], replicated
- zero_proj: bfloat16 [17, 384, 384], replicated
- hint_proj: bfloat16 [384, 384], replicated
- skip_proj: bfloat16 [16, 768, 384], replicated
- final_norm: bfloat16 [2, 384], replicated
- w_out: bfloat16 [384, 384], replicated
Outputs:
- output: bfloat16 [4096, 384], P(('data', 'group')), parts along dimension 0
There are 4 independent parts. The reference program is written for one: setup_inputs(seed, part) draws one part's arguments, and reference() takes and returns one part's arrays. A program takes and returns all parts, laid end to end along the dimension named above; an argument that names none is the same for every part.
All inputs are finite; a program needn't handle non-finite values.
Results may differ from the reference program's by a relative error of at most 0.02.
Values are sent between devices in bfloat16 or wider.
A program may use at most 768 MiB of HBM per device.

```python
import math
import jax
import jax.numpy as jnp
from jax import lax

TOKENS = 1024
WIDTH = 384
HEADS = 6
LAYERS = 16

HEAD_DIM = WIDTH // HEADS
IN_BLOCKS = LAYERS + 1
Q_GAIN = math.sqrt(max(1.0, math.log(TOKENS / 16.0)))
EPS = 1e-6


def draw_normal(rng_key, dim_sizes, std_scale):
    return (jax.random.normal(rng_key, dim_sizes, jnp.float32) * std_scale).astype(jnp.bfloat16)


def draw_qkv(rng_key, lead_dims):
    col_gain = jnp.concatenate([jnp.full((WIDTH,), Q_GAIN, jnp.float32), jnp.ones((2 * WIDTH,), jnp.float32)])
    raw_vals = jax.random.normal(rng_key, lead_dims + (WIDTH, 3 * WIDTH), jnp.float32)
    return (raw_vals * col_gain * WIDTH ** -0.5).astype(jnp.bfloat16)


def draw_norms(rng_key, lead_dims, row_count):
    centre = jnp.tile(jnp.array([1.0, 0.0], jnp.float32), row_count // 2)[:, None]
    raw_vals = jax.random.normal(rng_key, lead_dims + (row_count, WIDTH), jnp.float32)
    return (raw_vals * 0.2 + centre).astype(jnp.bfloat16)


def setup_inputs(seed: int = 0, part: int = 0) -> dict:
    part_keys = jax.random.split(jax.random.fold_in(jax.random.key(seed), part), 2)
    rng_keys = jax.random.split(jax.random.key(seed + 1), 15)
    in_lead = (2, IN_BLOCKS)
    out_lead = (LAYERS,)
    return {
        "latents": draw_normal(part_keys[0], (TOKENS, WIDTH), 1.0),
        "hint_embed": draw_normal(part_keys[1], (TOKENS, WIDTH), 1.0),
        "in_qkv": draw_qkv(rng_keys[0], in_lead),
        "in_proj": draw_normal(rng_keys[1], in_lead + (HEADS, HEAD_DIM, WIDTH), WIDTH ** -0.5),
        "in_up": draw_normal(rng_keys[2], in_lead + (WIDTH, 4 * WIDTH), WIDTH ** -0.5),
        "in_down": draw_normal(rng_keys[3], in_lead + (4 * WIDTH, WIDTH), (4 * WIDTH) ** -0.5),
        "in_norm": draw_norms(rng_keys[4], in_lead, 4),
        "out_qkv": draw_qkv(rng_keys[5], out_lead),
        "out_proj": draw_normal(rng_keys[6], out_lead + (HEADS, HEAD_DIM, WIDTH), WIDTH ** -0.5),
        "out_up": draw_normal(rng_keys[7], out_lead + (WIDTH, 4 * WIDTH), WIDTH ** -0.5),
        "out_down": draw_normal(rng_keys[8], out_lead + (4 * WIDTH, WIDTH), (4 * WIDTH) ** -0.5),
        "out_norm": draw_norms(rng_keys[9], out_lead, 4),
        "zero_proj": draw_normal(rng_keys[10], (IN_BLOCKS, WIDTH, WIDTH), 0.6 * WIDTH ** -0.5),
        "hint_proj": draw_normal(rng_keys[11], (WIDTH, WIDTH), WIDTH ** -0.5),
        "skip_proj": draw_normal(rng_keys[12], (LAYERS, 2 * WIDTH, WIDTH), (2 * WIDTH) ** -0.5),
        "final_norm": draw_norms(rng_keys[13], (), 2),
        "w_out": draw_normal(rng_keys[14], (WIDTH, WIDTH), WIDTH ** -0.5),
    }


def mat_f32(left_op, right_op):
    return jnp.dot(left_op, right_op, preferred_element_type=jnp.float32)


def layer_norm(values, norm_gain, norm_shift):
    wide_vals = values.astype(jnp.float32)
    centered = wide_vals - jnp.mean(wide_vals, axis=-1, keepdims=True)
    variance = jnp.mean(centered * centered, axis=-1, keepdims=True)
    normed = centered * lax.rsqrt(variance + EPS)
    return (normed * norm_gain.astype(jnp.float32) + norm_shift.astype(jnp.float32)).astype(jnp.bfloat16)


def head_attend(head_args):
    queries, key_rows, val_rows = head_args
    scores = mat_f32(queries, key_rows.T) * HEAD_DIM ** -0.5
    att_probs = jax.nn.softmax(scores, axis=-1).astype(jnp.bfloat16)
    return mat_f32(att_probs, val_rows).astype(jnp.bfloat16)


def transformer_block(residual, params):
    w_qkv, w_proj, w_up, w_down, norm_rows = params
    normed = layer_norm(residual, norm_rows[0], norm_rows[1])
    qkv_all = mat_f32(normed, w_qkv).astype(jnp.bfloat16)
    by_head = qkv_all.reshape(TOKENS, 3, HEADS, HEAD_DIM).transpose(1, 2, 0, 3)
    head_out = lax.map(head_attend, (by_head[0], by_head[1], by_head[2]))
    head_out = head_out.transpose(1, 0, 2).reshape(TOKENS, WIDTH)
    residual = (residual.astype(jnp.float32) + mat_f32(head_out, w_proj.reshape(WIDTH, WIDTH))).astype(jnp.bfloat16)
    normed = layer_norm(residual, norm_rows[2], norm_rows[3])
    hidden = jax.nn.gelu(mat_f32(normed, w_up), approximate=True).astype(jnp.bfloat16)
    return (residual.astype(jnp.float32) + mat_f32(hidden, w_down)).astype(jnp.bfloat16)


def reference(latents, hint_embed, in_qkv, in_proj, in_up, in_down, in_norm, out_qkv, out_proj, out_up, out_down, out_norm, zero_proj, hint_proj, skip_proj, final_norm, w_out):
    def in_step(residual, params):
        residual = transformer_block(residual, params)
        return residual, residual

    def out_step(residual, xs_pack):
        merged = mat_f32(jnp.concatenate([residual, xs_pack[6]], axis=-1), xs_pack[5]).astype(jnp.bfloat16)
        return transformer_block(merged, xs_pack[:5]), None

    ctrl_start = (latents.astype(jnp.float32) + mat_f32(hint_embed, hint_proj)).astype(jnp.bfloat16)
    base_params = (in_qkv[0], in_proj[0], in_up[0], in_down[0], in_norm[0])
    ctrl_params = (in_qkv[1], in_proj[1], in_up[1], in_down[1], in_norm[1])
    base_outs = lax.scan(in_step, latents, base_params)[1]
    ctrl_outs = lax.scan(in_step, ctrl_start, ctrl_params)[1]
    ctrl_res = jnp.einsum("bnd,bde->bne", ctrl_outs.astype(jnp.float32), zero_proj.astype(jnp.float32)).astype(jnp.bfloat16)
    sum_all = (base_outs.astype(jnp.float32) + ctrl_res.astype(jnp.float32)).astype(jnp.bfloat16)
    out_xs = (out_qkv, out_proj, out_up, out_down, out_norm, skip_proj, sum_all[:LAYERS][::-1])
    out_state = lax.scan(out_step, sum_all[LAYERS], out_xs)[0]
    normed = layer_norm(out_state, final_norm[0], final_norm[1])
    return mat_f32(normed, w_out).astype(jnp.bfloat16)
```

```python
import functools
import math

import jax
import jax.numpy as jnp
from jax import lax
from jax.experimental import pallas as pl
from jax.experimental.pallas import tpu as pltpu
from jax.sharding import PartitionSpec as P

EPS = 1e-6
MESH = pl.DeviceIdType.MESH
F32, BF16 = jnp.float32, jnp.bfloat16


def mat_f32(left_op, right_op):
    return jnp.dot(left_op, right_op, preferred_element_type=F32)


def mat_nt(left_op, right_op):
    return lax.dot_general(left_op, right_op, (((1,), (1,)), ((), ())), preferred_element_type=F32)


def norm_rows_of(values, gain, shift):
    wide = values.astype(F32)
    centered = wide - jnp.mean(wide, axis=-1, keepdims=True)
    variance = jnp.mean(centered * centered, axis=-1, keepdims=True)
    return (centered * lax.rsqrt(variance + EPS) * gain + shift).astype(BF16)


def gelu_tanh(v):
    k = math.sqrt(2.0 / math.pi)
    inner = v * (k + (k * 0.044715) * (v * v))
    half = 0.5 * v
    return half + half * jnp.tanh(inner)


def kernel(
    dims,
    x_ref, hint_ref, in_norm, out_norm, hint_proj, final_norm, w_out,
    in_qkv, in_proj, in_up, in_down, out_qkv, out_proj, out_up, out_down, zero_proj, skip_proj,
    y_ref,
    res, store, inbox, kv, qbuf, abuf, hbuf, s_buf, p_buf, l_buf, normf,
    wqkv, wproj, wup, wdown, wskip, zbuf, c0buf, ysend, yrecv,
    wsem, zsem, first_send, first_recv, kv_send, kv_recv, ctrl_send, box_recv, y_send, y_recv,
):
    group, n, slab, width, head_dim = dims
    n_in = n + 1
    slots = group // 2
    rows = slots * slab
    half = group // 2
    qc = rows // 2
    pair_w = 2 * head_dim
    pairs = width // pair_w
    scale = math.log2(math.e) * head_dim ** -0.5

    me = lax.axis_index("group")
    core = me % 2
    slot_me = me // 2
    base_dev = core
    ctrl_dev = half + core
    partner = me + 1 - 2 * core
    is_base = me < 2
    is_ctrl = (me >= half) & (me < half + 2)
    helper_of = 2 + 5 * core
    is_help = (me == 2) | (me == 7)
    help_core = (me == 7).astype(jnp.int32)
    branch = (me // half)

    def rcopy(src, dst, send, recv, dev):
        return pltpu.make_async_remote_copy(
            src_ref=src, dst_ref=dst, send_sem=send, recv_sem=recv, device_id={"group": dev}, device_id_type=MESH)

    barrier = pltpu.get_barrier_semaphore()
    for d in range(1, group):
        pl.semaphore_signal(barrier, inc=1, device_id={"group": (me + d) % group}, device_id_type=MESH)
    pl.semaphore_wait(barrier, group - 1)

    def w_copies(src5, idx, slot):
        out = []
        for k, (s, d) in enumerate(zip(src5, (wqkv, wproj, wup, wdown))):
            out.append(pltpu.make_async_copy(s.at[idx], d.at[slot], wsem.at[slot, k]))
        return out

    ins = (in_qkv, in_proj, in_up, in_down)
    outs = (out_qkv, out_proj, out_up, out_down)

    @pl.when(is_base | is_ctrl)
    def _():
        for c in w_copies(ins, (branch, 0), 0):
            c.start()

    slab_rows = pl.ds(pl.multiple_of(slot_me * slab, slab), slab)
    to_base = rcopy(x_ref, res.at[slab_rows], first_send.at[0], first_recv.at[slot_me], base_dev)

    @pl.when(jnp.logical_not(is_base))
    def _():
        to_base.start()

    c0buf[...] = (x_ref[...].astype(F32) + mat_f32(hint_ref[...], hint_proj[...])).astype(BF16)
    to_ctrl = rcopy(c0buf, res.at[slab_rows], first_send.at[1], first_recv.at[slot_me], ctrl_dev)

    @pl.when(jnp.logical_not(is_ctrl))
    def _():
        to_ctrl.start()

    @pl.when(is_base)
    def _():
        res[slab_rows, :] = x_ref[...]

    @pl.when(is_ctrl)
    def _():
        res[slab_rows, :] = c0buf[...]

    @pl.when(is_base | is_ctrl)
    def _():
        for s in range(slots):
            @pl.when(s != slot_me)
            def _():
                blk = res.at[pl.ds(s * slab, slab)]
                rcopy(blk, blk, first_send.at[0], first_recv.at[s], me).wait_recv()

    def block(i):
        slot = i % 2

        @pl.when(i < n_in)
        def _():
            normf[...] = in_norm[branch, jnp.minimum(i, n_in - 1)].astype(F32)

        @pl.when(i >= n_in)
        def _():
            normf[...] = out_norm[jnp.maximum(i - n_in, 0)].astype(F32)

        g1, b1, g2, b2 = (normf[k:k + 1, :] for k in range(4))
        cps = w_copies(ins, (0, 0), slot)
        cps[0].wait()
        sends = []
        for c in range(2):
            r = slice(c * qc, (c + 1) * qc)
            t = norm_rows_of(res[r, :], g1, b1)
            kv[slot, r, :] = mat_f32(t, wqkv[slot, :, width:]).astype(BF16)
            cp = rcopy(kv.at[slot, pl.ds(c * qc, qc)], kv.at[slot, pl.ds(rows + c * qc, qc)],
                       kv_send.at[slot, c], kv_recv.at[slot, c], partner)
            cp.start()
            sends.append(cp)
            qbuf[r, :] = mat_f32(t, wqkv[slot, :, :width]).astype(BF16)
        for cp in sends:
            cp.wait_recv()
        low = lax.broadcasted_iota(jnp.int32, (qc, pair_w), 1) < head_dim
        unit = 0
        for c in range(2):
            r = slice(c * qc, (c + 1) * qc)
            for p in range(pairs):
                b = unit % 2
                unit += 1
                cols = slice(p * pair_w, (p + 1) * pair_w)
                vcols = slice(width + p * pair_w, width + (p + 1) * pair_w)
                q = qbuf[r, cols]
                zero = jnp.zeros_like(q)
                both = jnp.concatenate([jnp.where(low, q, zero), jnp.where(low, zero, q)], axis=0)
                s_buf[b] = mat_nt(both, kv[slot, :, cols])
                step = 64
                for rb in range(0, 2 * qc, step):
                    s = s_buf[b, rb:rb + step, :]
                    m = jnp.max(s, axis=-1, keepdims=True)
                    e = jnp.exp2((s - m) * scale)
                    l = jnp.sum(e, axis=-1, keepdims=True)
                    p_buf[b, rb:rb + step, :] = e.astype(BF16)
                    l_buf[b, rb:rb + step, :] = jnp.broadcast_to(1.0 / l, (step, pair_w))
                o = mat_f32(p_buf[b], kv[slot, :, vcols]) * l_buf[b]
                abuf[r, cols] = jnp.where(low, o[:qc], o[qc:]).astype(BF16)
        for k in range(1, 4):
            cps[k].wait()
        for c in range(2):
            r = slice(c * qc, (c + 1) * qc)
            u = (res[r, :].astype(F32) + mat_f32(abuf[r, :], wproj[slot])).astype(BF16)
            t = norm_rows_of(u, g2, b2)
            hbuf[...] = gelu_tanh(mat_f32(t, wup[slot])).astype(BF16)
            res[r, :] = (u.astype(F32) + mat_f32(hbuf[...], wdown[slot])).astype(BF16)
        for cp in sends:
            cp.wait_send()

    n_iter = jnp.where(is_base, n_in + n, n_in)

    def c_send(i):
        return rcopy(store.at[i], inbox.at[i], ctrl_send.at[i], box_recv.at[i], helper_of)

    def box_wait(i):
        rcopy(inbox.at[i], inbox.at[i], ctrl_send.at[i], box_recv.at[i], me).wait_recv()

    def layer(i, carry):
        nxt = i + 1

        @pl.when(nxt < n_in)
        def _():
            for c in w_copies(ins, (branch, jnp.minimum(nxt, n_in - 1)), nxt % 2):
                c.start()

        @pl.when((nxt >= n_in) & (nxt < n_iter))
        def _():
            j = jnp.clip(nxt - n_in, 0, n - 1)
            for c in w_copies(outs, j, nxt % 2):
                c.start()
            pltpu.make_async_copy(skip_proj.at[j], wskip.at[nxt % 2], wsem.at[nxt % 2, 4]).start()

        @pl.when(i == n_in)
        def _():
            box_wait(n)
            res[...] = (res[...].astype(F32) + inbox[n].astype(F32)).astype(BF16)

        @pl.when(i >= n_in)
        def _():
            src = jnp.clip(n - 1 - (i - n_in), 0, n - 1)
            box_wait(src)
            slot = i % 2
            pltpu.make_async_copy(skip_proj.at[0], wskip.at[slot], wsem.at[slot, 4]).wait()
            for c in range(2):
                r = slice(c * qc, (c + 1) * qc)
                sk = (store[src, r, :].astype(F32) + inbox[src, r, :].astype(F32)).astype(BF16)
                top = mat_f32(res[r, :], wskip[slot, :width, :])
                res[r, :] = (top + mat_f32(sk, wskip[slot, width:, :])).astype(BF16)

        block(i)

        @pl.when(i < n_in)
        def _():
            ii = jnp.minimum(i, n)
            store[ii] = res[...]

            @pl.when(is_ctrl)
            def _():
                c_send(ii).start()

        return carry

    @pl.when(is_base | is_ctrl)
    def _():
        lax.fori_loop(0, n_iter, layer, 0)

    @pl.when(is_ctrl)
    def _():
        lax.fori_loop(0, n_in, lambda i, a: (c_send(i).wait_send(), a)[1], 0)

    @pl.when(is_help)
    def _():
        def z_copy(i):
            return pltpu.make_async_copy(zero_proj.at[i], zbuf.at[i % 2], zsem.at[i % 2])

        def r_send(i):
            return rcopy(store.at[i], inbox.at[i], ctrl_send.at[i], box_recv.at[i], help_core)

        z_copy(0).start()

        def step(i, a):
            @pl.when(i + 1 < n_in)
            def _():
                z_copy(jnp.minimum(i + 1, n)).start()

            z_copy(i).wait()
            box_wait(i)
            for c in range(2):
                r = slice(c * qc, (c + 1) * qc)
                store[i, r, :] = mat_f32(inbox[i, r, :], zbuf[i % 2]).astype(BF16)
            r_send(i).start()
            return a

        lax.fori_loop(0, n_in, step, 0)
        lax.fori_loop(0, n_in, lambda i, a: (r_send(i).wait_send(), a)[1], 0)

    @pl.when(is_base)
    def _():
        gf, bf = final_norm[0:1, :].astype(F32), final_norm[1:2, :].astype(F32)
        copies = []
        for s in range(slots):
            t = norm_rows_of(res[s * slab:(s + 1) * slab, :], gf, bf)
            y = mat_f32(t, w_out[...]).astype(BF16)
            if s == 0:
                y_ref[...] = y
            else:
                ysend[s] = y
                cp = rcopy(ysend.at[s], yrecv, y_send.at[s], y_recv, 2 * s + core)
                cp.start()
                copies.append(cp)
        for cp in copies:
            cp.wait_send()

    @pl.when(jnp.logical_not(is_base))
    def _():
        to_base.wait_send()
        rcopy(yrecv, yrecv, y_send.at[0], y_recv, me).wait_recv()
        y_ref[...] = yrecv[...]

    @pl.when(jnp.logical_not(is_ctrl))
    def _():
        to_ctrl.wait_send()


def solution(mesh):
    group = mesh.shape["group"]

    def device_step(x_own, hint_own, in_qkv, in_proj, in_up, in_down, in_norm, out_qkv, out_proj, out_up, out_down, out_norm, zero_proj, hint_proj, skip_proj, final_norm, w_out):
        slab, width = x_own.shape
        n = skip_proj.shape[0]
        heads, head_dim = in_proj.shape[2], in_proj.shape[3]
        hidden = in_up.shape[-1]
        rows = (group // 2) * slab
        qc = rows // 2
        in_proj = in_proj.reshape(in_proj.shape[:2] + (width, width))
        out_proj = out_proj.reshape(out_proj.shape[:1] + (width, width))
        vm = pl.BlockSpec(memory_space=pltpu.VMEM)
        hb = pl.BlockSpec(memory_space=pl.ANY)
        dma = pltpu.SemaphoreType.DMA
        return pl.pallas_call(
            functools.partial(kernel, (group, n, slab, width, head_dim)),
            out_shape=jax.ShapeDtypeStruct((slab, width), BF16),
            in_specs=[vm] * 7 + [hb] * 10,
            out_specs=vm,
            scratch_shapes=[
                pltpu.VMEM((rows, width), BF16),
                pltpu.VMEM((n + 1, rows, width), BF16),
                pltpu.VMEM((n + 1, rows, width), BF16),
                pltpu.VMEM((2, 2 * rows, 2 * width), BF16),
                pltpu.VMEM((rows, width), BF16),
                pltpu.VMEM((rows, width), BF16),
                pltpu.VMEM((qc, hidden), BF16),
                pltpu.VMEM((2, 2 * qc, 2 * rows), F32),
                pltpu.VMEM((2, 2 * qc, 2 * rows), BF16),
                pltpu.VMEM((2, 2 * qc, 2 * head_dim), F32),
                pltpu.VMEM((4, width), F32),
                pltpu.VMEM((2, width, 3 * width), BF16),
                pltpu.VMEM((2, width, width), BF16),
                pltpu.VMEM((2, width, hidden), BF16),
                pltpu.VMEM((2, hidden, width), BF16),
                pltpu.VMEM((2, 2 * width, width), BF16),
                pltpu.VMEM((2, width, width), BF16),
                pltpu.VMEM((slab, width), BF16),
                pltpu.VMEM((group // 2, slab, width), BF16),
                pltpu.VMEM((slab, width), BF16),
                dma((2, 5)), dma((2,)),
                dma((2,)), dma((group // 2,)),
                dma((2, 2)), dma((2, 2)),
                dma((n + 1,)), dma((n + 1,)),
                dma((group // 2,)), dma,
            ],
            compiler_params=pltpu.CompilerParams(
                collective_id=0, has_side_effects=True, vmem_limit_bytes=60 * 1024 * 1024),
        )(x_own, hint_own, in_norm, out_norm, hint_proj, final_norm, w_out,
          in_qkv, in_proj, in_up, in_down, out_qkv, out_proj, out_up, out_down, zero_proj, skip_proj)

    tok_spec = P(("data", "group"), None)
    return jax.shard_map(device_step, mesh=mesh, in_specs=(tok_spec, tok_spec) + (P(),) * 15, out_specs=tok_spec, check_vma=False)
```

```python
import functools
import math

import jax
import jax.numpy as jnp
from jax import lax
from jax.experimental import pallas as pl
from jax.experimental.pallas import tpu as pltpu
from jax.sharding import PartitionSpec as P

EPS = 1e-6
WAIT_AT = 4
MESH = pl.DeviceIdType.MESH
F32, BF16 = jnp.float32, jnp.bfloat16


def mat_f32(left_op, right_op):
    return jnp.dot(left_op, right_op, preferred_element_type=F32)


def mat_nt(left_op, right_op):
    return lax.dot_general(left_op, right_op, (((1,), (1,)), ((), ())), preferred_element_type=F32)


def norm_rows_of(values, gain, shift):
    wide = values.astype(F32)
    centered = wide - jnp.mean(wide, axis=-1, keepdims=True)
    variance = jnp.mean(centered * centered, axis=-1, keepdims=True)
    return (centered * lax.rsqrt(variance + EPS) * gain + shift).astype(BF16)


def gelu_tanh(v):
    k = math.sqrt(2.0 / math.pi)
    inner = v * (k + (k * 0.044715) * (v * v))
    half = 0.5 * v
    return half + half * jnp.tanh(inner)


def kernel(
    dims,
    x_ref, hint_ref, in_norm, out_norm, hint_proj, final_norm, w_out,
    in_qkv, in_proj, in_up, in_down, out_qkv, out_proj, out_up, out_down, zero_proj, skip_proj,
    y_ref,
    res, store, inbox, kk, vt, qbuf, abuf, hbuf, s_buf, p_buf, obuf, ml_buf, normf,
    wqkv, wproj, wup, wdown, wskip, zbuf, c0buf, ysend, yrecv,
    wsem, zsem, first_send, first_recv, kv_send, kv_recv, ctrl_send, box_recv, y_send, y_recv,
):
    group, n, slab, width, head_dim = dims
    n_in = n + 1
    slots = group // 2
    rows = slots * slab
    half = group // 2
    qc = rows // 2
    pair_w = 2 * head_dim
    pairs = width // pair_w
    scale = math.log2(math.e) * head_dim ** -0.5

    me = lax.axis_index("group")
    core = me % 2
    slot_me = me // 2
    base_dev = core
    ctrl_dev = half + core
    partner = me + 1 - 2 * core
    is_base = me < 2
    is_ctrl = (me >= half) & (me < half + 2)
    helper_of = 2 + 5 * core
    is_help = (me == 2) | (me == 7)
    help_core = (me == 7).astype(jnp.int32)
    branch = (me // half)

    def rcopy(src, dst, send, recv, dev):
        return pltpu.make_async_remote_copy(
            src_ref=src, dst_ref=dst, send_sem=send, recv_sem=recv, device_id={"group": dev}, device_id_type=MESH)

    barrier = pltpu.get_barrier_semaphore()
    for d in range(1, group):
        pl.semaphore_signal(barrier, inc=1, device_id={"group": (me + d) % group}, device_id_type=MESH)
    pl.semaphore_wait(barrier, group - 1)

    def w_copies(src5, idx, slot):
        out = []
        for k, (s, d) in enumerate(zip(src5, (wqkv, wproj, wup, wdown))):
            out.append(pltpu.make_async_copy(s.at[idx], d.at[slot], wsem.at[slot, k]))
        return out

    ins = (in_qkv, in_proj, in_up, in_down)
    outs = (out_qkv, out_proj, out_up, out_down)

    @pl.when(is_base | is_ctrl)
    def _():
        for c in w_copies(ins, (branch, 0), 0):
            c.start()

    slab_rows = pl.ds(pl.multiple_of(slot_me * slab, slab), slab)
    to_base = rcopy(x_ref, res.at[slab_rows], first_send.at[0], first_recv.at[slot_me], base_dev)

    @pl.when(jnp.logical_not(is_base))
    def _():
        to_base.start()

    c0buf[...] = (x_ref[...].astype(F32) + mat_f32(hint_ref[...], hint_proj[...])).astype(BF16)
    to_ctrl = rcopy(c0buf, res.at[slab_rows], first_send.at[1], first_recv.at[slot_me], ctrl_dev)

    @pl.when(jnp.logical_not(is_ctrl))
    def _():
        to_ctrl.start()

    @pl.when(is_base)
    def _():
        res[slab_rows, :] = x_ref[...]

    @pl.when(is_ctrl)
    def _():
        res[slab_rows, :] = c0buf[...]

    @pl.when(is_base | is_ctrl)
    def _():
        for s in range(slots):
            @pl.when(s != slot_me)
            def _():
                blk = res.at[pl.ds(s * slab, slab)]
                rcopy(blk, blk, first_send.at[0], first_recv.at[s], me).wait_recv()

    def block(i):
        slot = i % 2

        @pl.when(i < n_in)
        def _():
            normf[...] = in_norm[branch, jnp.minimum(i, n_in - 1)].astype(F32)

        @pl.when(i >= n_in)
        def _():
            normf[...] = out_norm[jnp.maximum(i - n_in, 0)].astype(F32)

        g1, b1, g2, b2 = (normf[k:k + 1, :] for k in range(4))
        cps = w_copies(ins, (0, 0), slot)
        for cp in cps:
            cp.wait()
        t = norm_rows_of(res[...], g1, b1)
        kk[slot, 0] = mat_f32(t, wqkv[slot, :, width:2 * width]).astype(BF16)
        vt[slot, 0] = lax.dot_general(wqkv[slot, :, 2 * width:], t, (((0,), (1,)), ((), ())), preferred_element_type=F32).astype(BF16)
        sends = []
        for k, buf in enumerate((kk, vt)):
            cp = rcopy(buf.at[slot, 0], buf.at[slot, 1], kv_send.at[slot, k], kv_recv.at[slot, k], partner)
            cp.start()
            sends.append(cp)
        q = mat_f32(t, wqkv[slot, :, :width]).astype(BF16)
        low = lax.broadcasted_iota(jnp.int32, (rows, width), 1) % pair_w < head_dim
        qbuf[0] = jnp.where(low, q, jnp.zeros_like(q))
        qbuf[1] = jnp.where(low, jnp.zeros_like(q), q)

        units = [(c, p) for c in range(2) for p in range(pairs)]
        step = 128

        def scores(part, u):
            c, p = units[u]
            cols = slice(p * pair_w, (p + 1) * pair_w)
            both = jnp.concatenate([qbuf[0, c * qc:(c + 1) * qc, cols], qbuf[1, c * qc:(c + 1) * qc, cols]], axis=0)
            s_buf[u % 2] = mat_nt(kk[slot, part, :, cols], both)

        def fold(v, op):
            return op(v.reshape(-1, 8, v.shape[-1]), axis=0)

        def soften(part, u):
            c, p = units[u]
            b = u % 2
            r = slice(c * qc, (c + 1) * qc)
            st = 2 * u
            m8 = fold(s_buf[b, 0:step, :], jnp.max)
            for rb in range(step, rows, step):
                m8 = jnp.maximum(m8, fold(s_buf[b, rb:rb + step, :], jnp.max))
            m = jnp.max(m8, axis=0, keepdims=True)
            if part == 1:
                m_old, l_old = ml_buf[st:st + 1, :], ml_buf[st + 1:st + 2, :]
                m = jnp.maximum(m, m_old)
                fix = jnp.exp2((m_old - m) * scale)
            m8 = jnp.broadcast_to(m, m8.shape)
            l8 = jnp.zeros_like(m8)
            for rb in range(0, rows, step):
                s3 = s_buf[b, rb:rb + step, :].reshape(step // 8, 8, 2 * qc)
                e = jnp.exp2((s3 - m8[None]) * scale)
                p_buf[b, rb:rb + step, :] = e.reshape(step, 2 * qc).astype(BF16)
                l8 = l8 + jnp.sum(e, axis=0)
                m8 = jnp.where(l8 >= 0.0, m8, l8)
            l = jnp.sum(l8, axis=0, keepdims=True)
            if part == 0:
                ml_buf[st:st + 1, :] = m
                ml_buf[st + 1:st + 2, :] = l
            else:
                inv = 1.0 / (l + l_old * fix)
            for hh in range(2):
                lanes = slice(hh * qc, (hh + 1) * qc)
                h = 2 * p + hh
                hr = slice(h * head_dim, (h + 1) * head_dim)
                o = mat_f32(vt[slot, part, hr, :], p_buf[b, :, lanes])
                if part == 0:
                    obuf[hr, r] = o
                else:
                    abuf[hr, r] = ((o + obuf[hr, r] * fix[:, lanes]) * inv[:, lanes]).astype(BF16)

        order = [(part, u) for part in range(2) for u in range(len(units))]
        scores(*order[0])
        for k, (part, u) in enumerate(order):
            if k == WAIT_AT:
                for cp in sends:
                    cp.wait_recv()
            if k + 1 < len(order):
                scores(*order[k + 1])
            soften(part, u)
        for c in range(2):
            r = slice(c * qc, (c + 1) * qc)
            u = (res[r, :].astype(F32) + lax.dot_general(abuf[:, r], wproj[slot], (((0,), (0,)), ((), ())), preferred_element_type=F32)).astype(BF16)
            t = norm_rows_of(u, g2, b2)
            hbuf[...] = gelu_tanh(mat_f32(t, wup[slot])).astype(BF16)
            res[r, :] = (u.astype(F32) + mat_f32(hbuf[...], wdown[slot])).astype(BF16)
        for cp in sends:
            cp.wait_send()

    n_iter = jnp.where(is_base, n_in + n, n_in)

    def c_send(i):
        return rcopy(store.at[i], inbox.at[i], ctrl_send.at[i], box_recv.at[i], helper_of)

    def box_wait(i):
        rcopy(inbox.at[i], inbox.at[i], ctrl_send.at[i], box_recv.at[i], me).wait_recv()

    def layer(i, carry):
        nxt = i + 1

        @pl.when(nxt < n_in)
        def _():
            for c in w_copies(ins, (branch, jnp.minimum(nxt, n_in - 1)), nxt % 2):
                c.start()

        @pl.when((nxt >= n_in) & (nxt < n_iter))
        def _():
            j = jnp.clip(nxt - n_in, 0, n - 1)
            for c in w_copies(outs, j, nxt % 2):
                c.start()
            pltpu.make_async_copy(skip_proj.at[j], wskip.at[nxt % 2], wsem.at[nxt % 2, 4]).start()

        @pl.when(i == n_in)
        def _():
            box_wait(n)
            res[...] = (res[...].astype(F32) + inbox[n].astype(F32)).astype(BF16)

        @pl.when(i >= n_in)
        def _():
            src = jnp.clip(n - 1 - (i - n_in), 0, n - 1)
            box_wait(src)
            slot = i % 2
            pltpu.make_async_copy(skip_proj.at[0], wskip.at[slot], wsem.at[slot, 4]).wait()
            for c in range(2):
                r = slice(c * qc, (c + 1) * qc)
                sk = (store[src, r, :].astype(F32) + inbox[src, r, :].astype(F32)).astype(BF16)
                top = mat_f32(res[r, :], wskip[slot, :width, :])
                res[r, :] = (top + mat_f32(sk, wskip[slot, width:, :])).astype(BF16)

        block(i)

        @pl.when(i < n_in)
        def _():
            ii = jnp.minimum(i, n)
            store[ii] = res[...]

            @pl.when(is_ctrl)
            def _():
                c_send(ii).start()

        return carry

    @pl.when(is_base | is_ctrl)
    def _():
        lax.fori_loop(0, n_iter, layer, 0)

    @pl.when(is_ctrl)
    def _():
        lax.fori_loop(0, n_in, lambda i, a: (c_send(i).wait_send(), a)[1], 0)

    @pl.when(is_help)
    def _():
        def z_copy(i):
            return pltpu.make_async_copy(zero_proj.at[i], zbuf.at[i % 2], zsem.at[i % 2])

        def r_send(i):
            return rcopy(store.at[i], inbox.at[i], ctrl_send.at[i], box_recv.at[i], help_core)

        z_copy(0).start()

        def step(i, a):
            @pl.when(i + 1 < n_in)
            def _():
                z_copy(jnp.minimum(i + 1, n)).start()

            z_copy(i).wait()
            box_wait(i)
            for c in range(2):
                r = slice(c * qc, (c + 1) * qc)
                store[i, r, :] = mat_f32(inbox[i, r, :], zbuf[i % 2]).astype(BF16)
            r_send(i).start()
            return a

        lax.fori_loop(0, n_in, step, 0)
        lax.fori_loop(0, n_in, lambda i, a: (r_send(i).wait_send(), a)[1], 0)

    @pl.when(is_base)
    def _():
        gf, bf = final_norm[0:1, :].astype(F32), final_norm[1:2, :].astype(F32)
        copies = []
        for s in range(slots):
            t = norm_rows_of(res[s * slab:(s + 1) * slab, :], gf, bf)
            y = mat_f32(t, w_out[...]).astype(BF16)
            if s == 0:
                y_ref[...] = y
            else:
                ysend[s] = y
                cp = rcopy(ysend.at[s], yrecv, y_send.at[s], y_recv, 2 * s + core)
                cp.start()
                copies.append(cp)
        for cp in copies:
            cp.wait_send()

    @pl.when(jnp.logical_not(is_base))
    def _():
        to_base.wait_send()
        rcopy(yrecv, yrecv, y_send.at[0], y_recv, me).wait_recv()
        y_ref[...] = yrecv[...]

    @pl.when(jnp.logical_not(is_ctrl))
    def _():
        to_ctrl.wait_send()


def solution(mesh):
    group = mesh.shape["group"]

    def device_step(x_own, hint_own, in_qkv, in_proj, in_up, in_down, in_norm, out_qkv, out_proj, out_up, out_down, out_norm, zero_proj, hint_proj, skip_proj, final_norm, w_out):
        slab, width = x_own.shape
        n = skip_proj.shape[0]
        heads, head_dim = in_proj.shape[2], in_proj.shape[3]
        hidden = in_up.shape[-1]
        rows = (group // 2) * slab
        qc = rows // 2
        in_proj = in_proj.reshape(in_proj.shape[:2] + (width, width))
        out_proj = out_proj.reshape(out_proj.shape[:1] + (width, width))
        vm = pl.BlockSpec(memory_space=pltpu.VMEM)
        hb = pl.BlockSpec(memory_space=pl.ANY)
        dma = pltpu.SemaphoreType.DMA
        return pl.pallas_call(
            functools.partial(kernel, (group, n, slab, width, head_dim)),
            out_shape=jax.ShapeDtypeStruct((slab, width), BF16),
            in_specs=[vm] * 7 + [hb] * 10,
            out_specs=vm,
            scratch_shapes=[
                pltpu.VMEM((rows, width), BF16),
                pltpu.VMEM((n + 1, rows, width), BF16),
                pltpu.VMEM((n + 1, rows, width), BF16),
                pltpu.VMEM((2, 2, rows, width), BF16),
                pltpu.VMEM((2, 2, width, rows), BF16),
                pltpu.VMEM((2, rows, width), BF16),
                pltpu.VMEM((width, rows), BF16),
                pltpu.VMEM((qc, hidden), BF16),
                pltpu.VMEM((2, rows, 2 * qc), F32),
                pltpu.VMEM((2, rows, 2 * qc), BF16),
                pltpu.VMEM((width, rows), F32),
                pltpu.VMEM((2 * heads, 2 * qc), F32),
                pltpu.VMEM((4, width), F32),
                pltpu.VMEM((2, width, 3 * width), BF16),
                pltpu.VMEM((2, width, width), BF16),
                pltpu.VMEM((2, width, hidden), BF16),
                pltpu.VMEM((2, hidden, width), BF16),
                pltpu.VMEM((2, 2 * width, width), BF16),
                pltpu.VMEM((2, width, width), BF16),
                pltpu.VMEM((slab, width), BF16),
                pltpu.VMEM((group // 2, slab, width), BF16),
                pltpu.VMEM((slab, width), BF16),
                dma((2, 5)), dma((2,)),
                dma((2,)), dma((group // 2,)),
                dma((2, 2)), dma((2, 2)),
                dma((n + 1,)), dma((n + 1,)),
                dma((group // 2,)), dma,
            ],
            compiler_params=pltpu.CompilerParams(
                collective_id=0, has_side_effects=True, vmem_limit_bytes=60 * 1024 * 1024),
        )(x_own, hint_own, in_norm, out_norm, hint_proj, final_norm, w_out,
          in_qkv, in_proj, in_up, in_down, out_qkv, out_proj, out_up, out_down, zero_proj, skip_proj)

    tok_spec = P(("data", "group"), None)
    return jax.shard_map(device_step, mesh=mesh, in_specs=(tok_spec, tok_spec) + (P(),) * 15, out_specs=tok_spec, check_vma=False)
```

```python
import functools
import math

import jax
import jax.numpy as jnp
from jax import lax
from jax.experimental import pallas as pl
from jax.experimental.pallas import tpu as pltpu
from jax.sharding import PartitionSpec as P

EPS = 1e-6
FILL = 9
WAIT_K, WAIT_V = 5, 6
MESH = pl.DeviceIdType.MESH
F32, BF16 = jnp.float32, jnp.bfloat16


def mat_f32(left_op, right_op):
    return jnp.dot(left_op, right_op, preferred_element_type=F32)


def mat_nt(left_op, right_op):
    return lax.dot_general(left_op, right_op, (((1,), (1,)), ((), ())), preferred_element_type=F32)


def norm_rows_of(values, gain, shift):
    wide = values.astype(F32)
    centered = wide - jnp.mean(wide, axis=-1, keepdims=True)
    variance = jnp.mean(centered * centered, axis=-1, keepdims=True)
    return (centered * lax.rsqrt(variance + EPS) * gain + shift).astype(BF16)


def gelu_tanh(v):
    k = math.sqrt(2.0 / math.pi)
    inner = v * (k + (k * 0.044715) * (v * v))
    half = 0.5 * v
    return half + half * jnp.tanh(inner)


def kernel(
    dims,
    x_ref, hint_ref, in_norm, out_norm, hint_proj, final_norm, w_out,
    in_qkv, in_proj, in_up, in_down, out_qkv, out_proj, out_up, out_down, zero_proj, skip_proj,
    y_ref,
    res, store, inbox, kk, vt, qbuf, abuf, hbuf, s_buf, p_buf, obuf, ml_buf, tbuf, normf,
    wqkv, wproj, wup, wdown, wskip, zbuf, c0buf, ysend, yrecv,
    wsem, zsem, first_send, first_recv, kv_send, kv_recv, ctrl_send, box_recv, y_send, y_recv,
):
    group, n, slab, width, head_dim = dims
    n_in = n + 1
    slots = group // 2
    rows = slots * slab
    half = group // 2
    qc = rows // 2
    pair_w = 2 * head_dim
    pairs = width // pair_w
    scale = math.log2(math.e) * head_dim ** -0.5

    me = lax.axis_index("group")
    core = me % 2
    slot_me = me // 2
    base_dev = core
    ctrl_dev = half + core
    partner = me + 1 - 2 * core
    is_base = me < 2
    is_ctrl = (me >= half) & (me < half + 2)
    helper_of = 2 + 5 * core
    is_help = (me == 2) | (me == 7)
    help_core = (me == 7).astype(jnp.int32)
    branch = (me // half)

    def rcopy(src, dst, send, recv, dev):
        return pltpu.make_async_remote_copy(
            src_ref=src, dst_ref=dst, send_sem=send, recv_sem=recv, device_id={"group": dev}, device_id_type=MESH)

    barrier = pltpu.get_barrier_semaphore()
    for d in range(1, group):
        pl.semaphore_signal(barrier, inc=1, device_id={"group": (me + d) % group}, device_id_type=MESH)
    pl.semaphore_wait(barrier, group - 1)

    def w_copies(src5, idx, slot):
        out = []
        for k, (s, d) in enumerate(zip(src5, (wqkv, wproj, wup, wdown))):
            out.append(pltpu.make_async_copy(s.at[idx], d.at[slot], wsem.at[slot, k]))
        return out

    ins = (in_qkv, in_proj, in_up, in_down)
    outs = (out_qkv, out_proj, out_up, out_down)

    @pl.when(is_base | is_ctrl)
    def _():
        for c in w_copies(ins, (branch, 0), 0):
            c.start()

    slab_rows = pl.ds(pl.multiple_of(slot_me * slab, slab), slab)
    to_base = rcopy(x_ref, res.at[slab_rows], first_send.at[0], first_recv.at[slot_me], base_dev)

    @pl.when(jnp.logical_not(is_base))
    def _():
        to_base.start()

    c0buf[...] = (x_ref[...].astype(F32) + mat_f32(hint_ref[...], hint_proj[...])).astype(BF16)
    to_ctrl = rcopy(c0buf, res.at[slab_rows], first_send.at[1], first_recv.at[slot_me], ctrl_dev)

    @pl.when(jnp.logical_not(is_ctrl))
    def _():
        to_ctrl.start()

    @pl.when(is_base)
    def _():
        res[slab_rows, :] = x_ref[...]

    @pl.when(is_ctrl)
    def _():
        res[slab_rows, :] = c0buf[...]

    @pl.when(is_base | is_ctrl)
    def _():
        for s in range(slots):
            @pl.when(s != slot_me)
            def _():
                blk = res.at[pl.ds(s * slab, slab)]
                rcopy(blk, blk, first_send.at[0], first_recv.at[s], me).wait_recv()

    def block(i):
        slot = i % 2

        @pl.when(i < n_in)
        def _():
            normf[...] = in_norm[branch, jnp.minimum(i, n_in - 1)].astype(F32)

        @pl.when(i >= n_in)
        def _():
            normf[...] = out_norm[jnp.maximum(i - n_in, 0)].astype(F32)

        g1, b1, g2, b2 = (normf[k:k + 1, :] for k in range(4))
        cps = w_copies(ins, (0, 0), slot)
        for cp in cps:
            cp.wait()
        t = norm_rows_of(res[...], g1, b1)
        kk[slot, 0] = mat_f32(t, wqkv[slot, :, width:2 * width]).astype(BF16)
        vt[slot, 0] = lax.dot_general(wqkv[slot, :, 2 * width:], t, (((0,), (1,)), ((), ())), preferred_element_type=F32).astype(BF16)
        sends = []
        for k, buf in enumerate((kk, vt)):
            cp = rcopy(buf.at[slot, 0], buf.at[slot, 1], kv_send.at[slot, k], kv_recv.at[slot, k], partner)
            cp.start()
            sends.append(cp)
        q = mat_f32(t, wqkv[slot, :, :width]).astype(BF16)
        low = lax.broadcasted_iota(jnp.int32, (rows, width), 1) % pair_w < head_dim
        qbuf[0] = jnp.where(low, q, jnp.zeros_like(q))
        qbuf[1] = jnp.where(low, jnp.zeros_like(q), q)

        units = [(c, p) for c in range(2) for p in range(pairs)]
        step = 128

        def scores(part, u):
            c, p = units[u]
            cols = slice(p * pair_w, (p + 1) * pair_w)
            both = jnp.concatenate([qbuf[0, c * qc:(c + 1) * qc, cols], qbuf[1, c * qc:(c + 1) * qc, cols]], axis=0)
            s_buf[u % 2] = mat_nt(kk[slot, part, :, cols], both)

        def fold(v, op):
            return op(v.reshape(-1, 8, v.shape[-1]), axis=0)

        def soften(part, u):
            c, p = units[u]
            b = u % 2
            r = slice(c * qc, (c + 1) * qc)
            st = 2 * u
            m8 = fold(s_buf[b, 0:step, :], jnp.max)
            for rb in range(step, rows, step):
                m8 = jnp.maximum(m8, fold(s_buf[b, rb:rb + step, :], jnp.max))
            m = jnp.max(m8, axis=0, keepdims=True)
            if part == 1:
                m_old, l_old = ml_buf[st:st + 1, :], ml_buf[st + 1:st + 2, :]
                m = jnp.maximum(m, m_old)
                fix = jnp.exp2((m_old - m) * scale)
            m8 = jnp.broadcast_to(m, m8.shape)
            l8 = jnp.zeros_like(m8)
            for rb in range(0, rows, step):
                s3 = s_buf[b, rb:rb + step, :].reshape(step // 8, 8, 2 * qc)
                e = jnp.exp2((s3 - m8[None]) * scale)
                p_buf[b, rb:rb + step, :] = e.reshape(step, 2 * qc).astype(BF16)
                l8 = l8 + jnp.sum(e, axis=0)
                m8 = jnp.where(l8 >= 0.0, m8, l8)
            l = jnp.sum(l8, axis=0, keepdims=True)
            if part == 0:
                ml_buf[st:st + 1, :] = m
                ml_buf[st + 1:st + 2, :] = l
            else:
                inv = 1.0 / (l + l_old * fix)
            for hh in range(2):
                lanes = slice(hh * qc, (hh + 1) * qc)
                h = 2 * p + hh
                hr = slice(h * head_dim, (h + 1) * head_dim)
                o = mat_f32(vt[slot, part, hr, :], p_buf[b, :, lanes])
                if part == 0:
                    obuf[hr, r] = o
                else:
                    abuf[hr, r] = ((o + obuf[hr, r] * fix[:, lanes]) * inv[:, lanes]).astype(BF16)

        def mid(c):
            r = slice(c * qc, (c + 1) * qc)
            add = lax.dot_general(abuf[:, r], wproj[slot], (((0,), (0,)), ((), ())), preferred_element_type=F32)
            u = (res[r, :].astype(F32) + add).astype(BF16)
            res[r, :] = u
            tbuf[r, :] = norm_rows_of(u, g2, b2)

        def up(c):
            r = slice(c * qc, (c + 1) * qc)
            hbuf[r, :] = gelu_tanh(mat_f32(tbuf[r, :], wup[slot])).astype(BF16)

        def down(c):
            r = slice(c * qc, (c + 1) * qc)
            res[r, :] = (res[r, :].astype(F32) + mat_f32(hbuf[r, :], wdown[slot])).astype(BF16)

        order = [(part, u) for part in range(2) for u in range(len(units))]
        scores(*order[0])
        for k, (part, u) in enumerate(order):
            if k == WAIT_K:
                sends[0].wait_recv()
            if k == WAIT_V:
                sends[1].wait_recv()
            if k + 1 < len(order):
                scores(*order[k + 1])
            if k == FILL:
                mid(0)
            if k == FILL + 1:
                up(0)
            soften(part, u)
        for k in range(len(order), FILL + 2):
            (mid if k == FILL else up)(0)
        down(0)
        mid(1)
        up(1)
        down(1)
        for cp in sends:
            cp.wait_send()

    n_iter = jnp.where(is_base, n_in + n, n_in)

    def c_send(i, k):
        rr = pl.ds(k * slab, slab)
        return rcopy(store.at[i, rr], inbox.at[i, rr], ctrl_send.at[i, k], box_recv.at[i, k], helper_of)

    def box_wait(i, k):
        blk = inbox.at[i, pl.ds(k * slab, slab)]
        rcopy(blk, blk, ctrl_send.at[i, k], box_recv.at[i, k], me).wait_recv()

    def layer(i, carry):
        nxt = i + 1

        @pl.when(nxt < n_in)
        def _():
            for c in w_copies(ins, (branch, jnp.minimum(nxt, n_in - 1)), nxt % 2):
                c.start()

        @pl.when((nxt >= n_in) & (nxt < n_iter))
        def _():
            j = jnp.clip(nxt - n_in, 0, n - 1)
            for c in w_copies(outs, j, nxt % 2):
                c.start()
            pltpu.make_async_copy(skip_proj.at[j], wskip.at[nxt % 2], wsem.at[nxt % 2, 4]).start()

        @pl.when(i == n_in)
        def _():
            for k in range(slots):
                box_wait(n, k)
            res[...] = (res[...].astype(F32) + inbox[n].astype(F32)).astype(BF16)

        @pl.when(i >= n_in)
        def _():
            src = jnp.clip(n - 1 - (i - n_in), 0, n - 1)
            for k in range(slots):
                box_wait(src, k)
            slot = i % 2
            pltpu.make_async_copy(skip_proj.at[0], wskip.at[slot], wsem.at[slot, 4]).wait()
            for c in range(2):
                r = slice(c * qc, (c + 1) * qc)
                sk = (store[src, r, :].astype(F32) + inbox[src, r, :].astype(F32)).astype(BF16)
                top = mat_f32(res[r, :], wskip[slot, :width, :])
                res[r, :] = (top + mat_f32(sk, wskip[slot, width:, :])).astype(BF16)

        block(i)

        @pl.when(i < n_in)
        def _():
            ii = jnp.minimum(i, n)
            store[ii] = res[...]

            @pl.when(is_ctrl)
            def _():
                for k in range(slots):
                    c_send(ii, k).start()

        return carry

    @pl.when(is_base | is_ctrl)
    def _():
        lax.fori_loop(0, n_iter, layer, 0)

    @pl.when(is_ctrl)
    def _():
        def drain(i, a):
            for k in range(slots):
                c_send(i, k).wait_send()
            return a

        lax.fori_loop(0, n_in, drain, 0)

    @pl.when(is_help)
    def _():
        def z_copy(i):
            return pltpu.make_async_copy(zero_proj.at[i], zbuf.at[i % 2], zsem.at[i % 2])

        def r_send(i, k):
            rr = pl.ds(k * slab, slab)
            return rcopy(store.at[i, rr], inbox.at[i, rr], ctrl_send.at[i, k], box_recv.at[i, k], help_core)

        z_copy(0).start()

        def relay(i, a):
            @pl.when(i + 1 < n_in)
            def _():
                z_copy(jnp.minimum(i + 1, n)).start()

            z_copy(i).wait()
            for k in range(slots):
                r = slice(k * slab, (k + 1) * slab)
                box_wait(i, k)
                store[i, r, :] = mat_f32(inbox[i, r, :], zbuf[i % 2]).astype(BF16)
                r_send(i, k).start()
            return a

        lax.fori_loop(0, n_in, relay, 0)

        def drain(i, a):
            for k in range(slots):
                r_send(i, k).wait_send()
            return a

        lax.fori_loop(0, n_in, drain, 0)

    @pl.when(is_base)
    def _():
        gf, bf = final_norm[0:1, :].astype(F32), final_norm[1:2, :].astype(F32)
        copies = []
        for s in range(slots):
            t = norm_rows_of(res[s * slab:(s + 1) * slab, :], gf, bf)
            y = mat_f32(t, w_out[...]).astype(BF16)
            if s == 0:
                y_ref[...] = y
            else:
                ysend[s] = y
                cp = rcopy(ysend.at[s], yrecv, y_send.at[s], y_recv, 2 * s + core)
                cp.start()
                copies.append(cp)
        for cp in copies:
            cp.wait_send()

    @pl.when(jnp.logical_not(is_base))
    def _():
        to_base.wait_send()
        rcopy(yrecv, yrecv, y_send.at[0], y_recv, me).wait_recv()
        y_ref[...] = yrecv[...]

    @pl.when(jnp.logical_not(is_ctrl))
    def _():
        to_ctrl.wait_send()


def solution(mesh):
    group = mesh.shape["group"]

    def device_step(x_own, hint_own, in_qkv, in_proj, in_up, in_down, in_norm, out_qkv, out_proj, out_up, out_down, out_norm, zero_proj, hint_proj, skip_proj, final_norm, w_out):
        slab, width = x_own.shape
        n = skip_proj.shape[0]
        heads, head_dim = in_proj.shape[2], in_proj.shape[3]
        hidden = in_up.shape[-1]
        rows = (group // 2) * slab
        qc = rows // 2
        in_proj = in_proj.reshape(in_proj.shape[:2] + (width, width))
        out_proj = out_proj.reshape(out_proj.shape[:1] + (width, width))
        vm = pl.BlockSpec(memory_space=pltpu.VMEM)
        hb = pl.BlockSpec(memory_space=pl.ANY)
        dma = pltpu.SemaphoreType.DMA
        return pl.pallas_call(
            functools.partial(kernel, (group, n, slab, width, head_dim)),
            out_shape=jax.ShapeDtypeStruct((slab, width), BF16),
            in_specs=[vm] * 7 + [hb] * 10,
            out_specs=vm,
            scratch_shapes=[
                pltpu.VMEM((rows, width), BF16),
                pltpu.VMEM((n + 1, rows, width), BF16),
                pltpu.VMEM((n + 1, rows, width), BF16),
                pltpu.VMEM((2, 2, rows, width), BF16),
                pltpu.VMEM((2, 2, width, rows), BF16),
                pltpu.VMEM((2, rows, width), BF16),
                pltpu.VMEM((width, rows), BF16),
                pltpu.VMEM((rows, hidden), BF16),
                pltpu.VMEM((2, rows, 2 * qc), F32),
                pltpu.VMEM((2, rows, 2 * qc), BF16),
                pltpu.VMEM((width, rows), F32),
                pltpu.VMEM((2 * heads, 2 * qc), F32),
                pltpu.VMEM((rows, width), BF16),
                pltpu.VMEM((4, width), F32),
                pltpu.VMEM((2, width, 3 * width), BF16),
                pltpu.VMEM((2, width, width), BF16),
                pltpu.VMEM((2, width, hidden), BF16),
                pltpu.VMEM((2, hidden, width), BF16),
                pltpu.VMEM((2, 2 * width, width), BF16),
                pltpu.VMEM((2, width, width), BF16),
                pltpu.VMEM((slab, width), BF16),
                pltpu.VMEM((group // 2, slab, width), BF16),
                pltpu.VMEM((slab, width), BF16),
                dma((2, 5)), dma((2,)),
                dma((2,)), dma((group // 2,)),
                dma((2, 2)), dma((2, 2)),
                dma((n + 1, group // 2)), dma((n + 1, group // 2)),
                dma((group // 2,)), dma,
            ],
            compiler_params=pltpu.CompilerParams(
                collective_id=0, has_side_effects=True, vmem_limit_bytes=60 * 1024 * 1024),
        )(x_own, hint_own, in_norm, out_norm, hint_proj, final_norm, w_out,
          in_qkv, in_proj, in_up, in_down, out_qkv, out_proj, out_up, out_down, zero_proj, skip_proj)

    tok_spec = P(("data", "group"), None)
    return jax.shard_map(device_step, mesh=mesh, in_specs=(tok_spec, tok_spec) + (P(),) * 15, out_specs=tok_spec, check_vma=False)
```

```python
import functools
import math

import jax
import jax.numpy as jnp
from jax import lax
from jax.experimental import pallas as pl
from jax.experimental.pallas import tpu as pltpu
from jax.sharding import PartitionSpec as P

EPS = 1e-6
FILL = 9
WAIT_K, WAIT_V = 5, 6
MESH = pl.DeviceIdType.MESH
F32, BF16 = jnp.float32, jnp.bfloat16


def mat_f32(left_op, right_op):
    return jnp.dot(left_op, right_op, preferred_element_type=F32)


def mat_nt(left_op, right_op):
    return lax.dot_general(left_op, right_op, (((1,), (1,)), ((), ())), preferred_element_type=F32)


def norm_rows_of(values, gain, shift):
    wide = values.astype(F32)
    centered = wide - jnp.mean(wide, axis=-1, keepdims=True)
    variance = jnp.mean(centered * centered, axis=-1, keepdims=True)
    return (centered * lax.rsqrt(variance + EPS) * gain + shift).astype(BF16)


def gelu_tanh(v):
    k = math.sqrt(2.0 / math.pi)
    inner = v * (k + (k * 0.044715) * (v * v))
    half = 0.5 * v
    return half + half * jnp.tanh(inner)


def kernel(
    dims,
    x_ref, hint_ref, in_norm, out_norm, hint_proj, final_norm, w_out,
    in_qkv, in_proj, in_up, in_down, out_qkv, out_proj, out_up, out_down, zero_proj, skip_proj,
    y_ref,
    res, store, inbox, kk, vt, qbuf, abuf, hbuf, s_buf, p_buf, obuf, ml_buf, tbuf, normf,
    wqkv, wproj, wup, wdown, wskip, zbuf, c0buf, ysend, yrecv,
    wsem, zsem, first_send, first_recv, kv_send, kv_recv, ctrl_send, box_recv, y_send, y_recv,
):
    group, n, slab, width, head_dim = dims
    n_in = n + 1
    slots = group // 2
    rows = slots * slab
    half = group // 2
    qc = rows // 2
    pair_w = 2 * head_dim
    pairs = width // pair_w
    scale = math.log2(math.e) * head_dim ** -0.5

    me = lax.axis_index("group")
    core = me % 2
    slot_me = me // 2
    base_dev = core
    ctrl_dev = half + core
    partner = me + 1 - 2 * core
    is_base = me < 2
    is_ctrl = (me >= half) & (me < half + 2)
    helper_of = 2 + 5 * core
    is_help = (me == 2) | (me == 7)
    help_core = (me == 7).astype(jnp.int32)
    branch = (me // half)

    def rcopy(src, dst, send, recv, dev):
        return pltpu.make_async_remote_copy(
            src_ref=src, dst_ref=dst, send_sem=send, recv_sem=recv, device_id={"group": dev}, device_id_type=MESH)

    barrier = pltpu.get_barrier_semaphore()
    for d in range(1, group):
        pl.semaphore_signal(barrier, inc=1, device_id={"group": (me + d) % group}, device_id_type=MESH)
    pl.semaphore_wait(barrier, group - 1)

    def w_copies(src5, idx, slot):
        out = []
        for k, (s, d) in enumerate(zip(src5, (wqkv, wproj, wup, wdown))):
            out.append(pltpu.make_async_copy(s.at[idx], d.at[slot], wsem.at[slot, k]))
        return out

    ins = (in_qkv, in_proj, in_up, in_down)
    outs = (out_qkv, out_proj, out_up, out_down)

    @pl.when(is_base | is_ctrl)
    def _():
        for c in w_copies(ins, (branch, 0), 0):
            c.start()

    slab_rows = pl.ds(pl.multiple_of(slot_me * slab, slab), slab)
    to_base = rcopy(x_ref, res.at[slab_rows], first_send.at[0], first_recv.at[slot_me], base_dev)

    @pl.when(jnp.logical_not(is_base))
    def _():
        to_base.start()

    c0buf[...] = (x_ref[...].astype(F32) + mat_f32(hint_ref[...], hint_proj[...])).astype(BF16)
    to_ctrl = rcopy(c0buf, res.at[slab_rows], first_send.at[1], first_recv.at[slot_me], ctrl_dev)

    @pl.when(jnp.logical_not(is_ctrl))
    def _():
        to_ctrl.start()

    @pl.when(is_base)
    def _():
        res[slab_rows, :] = x_ref[...]

    @pl.when(is_ctrl)
    def _():
        res[slab_rows, :] = c0buf[...]

    @pl.when(is_base | is_ctrl)
    def _():
        for s in range(slots):
            @pl.when(s != slot_me)
            def _():
                blk = res.at[pl.ds(s * slab, slab)]
                rcopy(blk, blk, first_send.at[0], first_recv.at[s], me).wait_recv()

    def block(i):
        slot = i % 2

        @pl.when(i < n_in)
        def _():
            normf[:4, :width] = in_norm[branch, jnp.minimum(i, n_in - 1)].astype(F32)

        @pl.when(i >= n_in)
        def _():
            normf[:4, :width] = out_norm[jnp.maximum(i - n_in, 0)].astype(F32)

        g1, b1, g2, b2 = (normf[k:k + 1, :width] for k in range(4))
        cps = w_copies(ins, (0, 0), slot)
        for cp in cps:
            cp.wait()
        t = norm_rows_of(res[...], g1, b1)
        kk[slot, 0] = mat_f32(t, wqkv[slot, :, width:2 * width]).astype(BF16)
        vt[slot, 0] = lax.dot_general(wqkv[slot, :, 2 * width:], t, (((0,), (1,)), ((), ())), preferred_element_type=F32).astype(BF16)
        sends = []
        for k, buf in enumerate((kk, vt)):
            cp = rcopy(buf.at[slot, 0], buf.at[slot, 1], kv_send.at[slot, k], kv_recv.at[slot, k], partner)
            cp.start()
            sends.append(cp)
        q = mat_f32(t, wqkv[slot, :, :width]).astype(BF16)
        low = lax.broadcasted_iota(jnp.int32, (rows, width), 1) % pair_w < head_dim
        qbuf[0] = jnp.where(low, q, jnp.zeros_like(q))
        qbuf[1] = jnp.where(low, jnp.zeros_like(q), q)

        units = [(c, p) for c in range(2) for p in range(pairs)]
        step = 256

        def scores(part, u):
            c, p = units[u]
            cols = slice(p * pair_w, (p + 1) * pair_w)
            both = jnp.concatenate([qbuf[0, c * qc:(c + 1) * qc, cols], qbuf[1, c * qc:(c + 1) * qc, cols]], axis=0)
            s_buf[u % 2] = mat_nt(kk[slot, part, :, cols], both)

        def fold(v, op):
            return op(v.reshape(-1, 8, v.shape[-1]), axis=0)

        def peak(part, u):
            b = u % 2
            m8 = fold(s_buf[b, 0:step, :], jnp.max)
            for rb in range(step, rows, step):
                m8 = jnp.maximum(m8, fold(s_buf[b, rb:rb + step, :], jnp.max))
            return jnp.max(m8, axis=0, keepdims=True)

        def soften(part, u, m):
            b = u % 2
            st = 2 * u
            fix = None
            if part == 1:
                m_old = ml_buf[st:st + 1, :]
                m = jnp.maximum(m, m_old)
                fix = jnp.exp2((m_old - m) * scale)
            m8 = jnp.broadcast_to(m, (8, 2 * qc))
            l8 = jnp.zeros_like(m8)
            for rb in range(0, rows, step):
                s3 = s_buf[b, rb:rb + step, :].reshape(step // 8, 8, 2 * qc)
                e = jnp.exp2((s3 - m8[None]) * scale)
                p_buf[b, rb:rb + step, :] = e.reshape(step, 2 * qc).astype(BF16)
                l8 = l8 + jnp.sum(e, axis=0)
                m8 = jnp.where(l8 >= 0.0, m8, l8)
            l = jnp.sum(l8, axis=0, keepdims=True)
            if part == 0:
                ml_buf[st:st + 1, :] = m
                ml_buf[st + 1:st + 2, :] = l
                return None, None
            return fix, 1.0 / (l + ml_buf[st + 1:st + 2, :] * fix)

        def weigh(part, u, fix, inv):
            c, p = units[u]
            b = u % 2
            r = slice(c * qc, (c + 1) * qc)
            for hh in range(2):
                lanes = slice(hh * qc, (hh + 1) * qc)
                h = 2 * p + hh
                hr = slice(h * head_dim, (h + 1) * head_dim)
                o = mat_f32(vt[slot, part, hr, :], p_buf[b, :, lanes])
                if part == 0:
                    obuf[hr, r] = o
                else:
                    abuf[hr, r] = ((o + obuf[hr, r] * fix[:, lanes]) * inv[:, lanes]).astype(BF16)

        def mid(c):
            r = slice(c * qc, (c + 1) * qc)
            add = lax.dot_general(abuf[:, r], wproj[slot], (((0,), (0,)), ((), ())), preferred_element_type=F32)
            u = (res[r, :].astype(F32) + add).astype(BF16)
            res[r, :] = u
            tbuf[r, :] = norm_rows_of(u, g2, b2)

        def up(c):
            r = slice(c * qc, (c + 1) * qc)
            hbuf[r, :] = gelu_tanh(mat_f32(tbuf[r, :], wup[slot])).astype(BF16)

        def down(c):
            r = slice(c * qc, (c + 1) * qc)
            res[r, :] = (res[r, :].astype(F32) + mat_f32(hbuf[r, :], wdown[slot])).astype(BF16)

        order = [(part, u) for part in range(2) for u in range(len(units))]
        scores(*order[0])
        m_next = peak(*order[0])
        for k, (part, u) in enumerate(order):
            if k == WAIT_K:
                sends[0].wait_recv()
            if k == WAIT_V:
                sends[1].wait_recv()
            m = m_next
            if k + 1 < len(order):
                scores(*order[k + 1])
                m_next = peak(*order[k + 1])
            if k == FILL:
                mid(0)
            if k == FILL + 1:
                up(0)
            weigh(part, u, *soften(part, u, m))
        for k in range(len(order), FILL + 2):
            (mid if k == FILL else up)(0)
        down(0)
        mid(1)
        up(1)
        down(1)
        for cp in sends:
            cp.wait_send()

    n_iter = jnp.where(is_base, n_in + n, n_in)

    def c_send(i, k):
        rr = pl.ds(k * slab, slab)
        return rcopy(store.at[i, rr], inbox.at[i, rr], ctrl_send.at[i, k], box_recv.at[i, k], helper_of)

    def box_wait(i, k):
        blk = inbox.at[i, pl.ds(k * slab, slab)]
        rcopy(blk, blk, ctrl_send.at[i, k], box_recv.at[i, k], me).wait_recv()

    def layer(i, carry):
        nxt = i + 1

        @pl.when(nxt < n_in)
        def _():
            for c in w_copies(ins, (branch, jnp.minimum(nxt, n_in - 1)), nxt % 2):
                c.start()

        @pl.when((nxt >= n_in) & (nxt < n_iter))
        def _():
            j = jnp.clip(nxt - n_in, 0, n - 1)
            for c in w_copies(outs, j, nxt % 2):
                c.start()
            pltpu.make_async_copy(skip_proj.at[j], wskip.at[nxt % 2], wsem.at[nxt % 2, 4]).start()

        @pl.when(i == n_in)
        def _():
            for k in range(slots):
                box_wait(n, k)
            res[...] = (res[...].astype(F32) + inbox[n].astype(F32)).astype(BF16)

        @pl.when(i >= n_in)
        def _():
            src = jnp.clip(n - 1 - (i - n_in), 0, n - 1)
            for k in range(slots):
                box_wait(src, k)
            slot = i % 2
            pltpu.make_async_copy(skip_proj.at[0], wskip.at[slot], wsem.at[slot, 4]).wait()
            for c in range(2):
                r = slice(c * qc, (c + 1) * qc)
                sk = (store[src, r, :].astype(F32) + inbox[src, r, :].astype(F32)).astype(BF16)
                top = mat_f32(res[r, :], wskip[slot, :width, :])
                res[r, :] = (top + mat_f32(sk, wskip[slot, width:, :])).astype(BF16)

        block(i)

        @pl.when(i < n_in)
        def _():
            ii = jnp.minimum(i, n)
            store[ii] = res[...]

            @pl.when(is_ctrl)
            def _():
                for k in range(slots):
                    c_send(ii, k).start()

        return carry

    @pl.when(is_base | is_ctrl)
    def _():
        lax.fori_loop(0, n_iter, layer, 0)

    @pl.when(is_ctrl)
    def _():
        def drain(i, a):
            for k in range(slots):
                c_send(i, k).wait_send()
            return a

        lax.fori_loop(0, n_in, drain, 0)

    @pl.when(is_help)
    def _():
        def z_copy(i):
            return pltpu.make_async_copy(zero_proj.at[i], zbuf.at[i % 2], zsem.at[i % 2])

        def r_send(i, k):
            rr = pl.ds(k * slab, slab)
            return rcopy(store.at[i, rr], inbox.at[i, rr], ctrl_send.at[i, k], box_recv.at[i, k], help_core)

        z_copy(0).start()

        def relay(i, a):
            @pl.when(i + 1 < n_in)
            def _():
                z_copy(jnp.minimum(i + 1, n)).start()

            z_copy(i).wait()
            for k in range(slots):
                r = slice(k * slab, (k + 1) * slab)
                box_wait(i, k)
                store[i, r, :] = mat_f32(inbox[i, r, :], zbuf[i % 2]).astype(BF16)
                r_send(i, k).start()
            return a

        lax.fori_loop(0, n_in, relay, 0)

        def drain(i, a):
            for k in range(slots):
                r_send(i, k).wait_send()
            return a

        lax.fori_loop(0, n_in, drain, 0)

    @pl.when(is_base)
    def _():
        gf, bf = final_norm[0:1, :].astype(F32), final_norm[1:2, :].astype(F32)
        copies = []
        for s in range(slots):
            t = norm_rows_of(res[s * slab:(s + 1) * slab, :], gf, bf)
            y = mat_f32(t, w_out[...]).astype(BF16)
            if s == 0:
                y_ref[...] = y
            else:
                ysend[s] = y
                cp = rcopy(ysend.at[s], yrecv, y_send.at[s], y_recv, 2 * s + core)
                cp.start()
                copies.append(cp)
        for cp in copies:
            cp.wait_send()

    @pl.when(jnp.logical_not(is_base))
    def _():
        to_base.wait_send()
        rcopy(yrecv, yrecv, y_send.at[0], y_recv, me).wait_recv()
        y_ref[...] = yrecv[...]

    @pl.when(jnp.logical_not(is_ctrl))
    def _():
        to_ctrl.wait_send()


def solution(mesh):
    group = mesh.shape["group"]

    def device_step(x_own, hint_own, in_qkv, in_proj, in_up, in_down, in_norm, out_qkv, out_proj, out_up, out_down, out_norm, zero_proj, hint_proj, skip_proj, final_norm, w_out):
        slab, width = x_own.shape
        n = skip_proj.shape[0]
        heads, head_dim = in_proj.shape[2], in_proj.shape[3]
        hidden = in_up.shape[-1]
        rows = (group // 2) * slab
        qc = rows // 2
        in_proj = in_proj.reshape(in_proj.shape[:2] + (width, width))
        out_proj = out_proj.reshape(out_proj.shape[:1] + (width, width))
        vm = pl.BlockSpec(memory_space=pltpu.VMEM)
        hb = pl.BlockSpec(memory_space=pl.ANY)
        dma = pltpu.SemaphoreType.DMA
        return pl.pallas_call(
            functools.partial(kernel, (group, n, slab, width, head_dim)),
            out_shape=jax.ShapeDtypeStruct((slab, width), BF16),
            in_specs=[vm] * 7 + [hb] * 10,
            out_specs=vm,
            scratch_shapes=[
                pltpu.VMEM((rows, width), BF16),
                pltpu.VMEM((n + 1, rows, width), BF16),
                pltpu.VMEM((n + 1, rows, width), BF16),
                pltpu.VMEM((2, 2, rows, width), BF16),
                pltpu.VMEM((2, 2, width, rows), BF16),
                pltpu.VMEM((2, rows, width), BF16),
                pltpu.VMEM((width, rows), BF16),
                pltpu.VMEM((rows, hidden), BF16),
                pltpu.VMEM((2, rows, 2 * qc), F32),
                pltpu.VMEM((2, rows, 2 * qc), BF16),
                pltpu.VMEM((width, rows), F32),
                pltpu.VMEM((2 * heads, 2 * qc), F32),
                pltpu.VMEM((rows, width), BF16),
                pltpu.VMEM((8, 2 * qc), F32),
                pltpu.VMEM((2, width, 3 * width), BF16),
                pltpu.VMEM((2, width, width), BF16),
                pltpu.VMEM((2, width, hidden), BF16),
                pltpu.VMEM((2, hidden, width), BF16),
                pltpu.VMEM((2, 2 * width, width), BF16),
                pltpu.VMEM((2, width, width), BF16),
                pltpu.VMEM((slab, width), BF16),
                pltpu.VMEM((group // 2, slab, width), BF16),
                pltpu.VMEM((slab, width), BF16),
                dma((2, 5)), dma((2,)),
                dma((2,)), dma((group // 2,)),
                dma((2, 2)), dma((2, 2)),
                dma((n + 1, group // 2)), dma((n + 1, group // 2)),
                dma((group // 2,)), dma,
            ],
            compiler_params=pltpu.CompilerParams(
                collective_id=0, has_side_effects=True, vmem_limit_bytes=60 * 1024 * 1024, internal_scratch_in_bytes=5 * 16384),
        )(x_own, hint_own, in_norm, out_norm, hint_proj, final_norm, w_out,
          in_qkv, in_proj, in_up, in_down, out_qkv, out_proj, out_up, out_down, zero_proj, skip_proj)

    tok_spec = P(("data", "group"), None)
    return jax.shard_map(device_step, mesh=mesh, in_specs=(tok_spec, tok_spec) + (P(),) * 15, out_specs=tok_spec, check_vma=False)
```

```python
import functools
import math

import jax
import jax.numpy as jnp
from jax import lax
from jax.experimental import pallas as pl
from jax.experimental.pallas import tpu as pltpu
from jax.sharding import PartitionSpec as P

EPS = 1e-6
STEP = 64
FILL = 6
MESH = pl.DeviceIdType.MESH
F32, BF16 = jnp.float32, jnp.bfloat16


def mat_f32(left_op, right_op):
    return jnp.dot(left_op, right_op, preferred_element_type=F32)


def mat_nt(left_op, right_op):
    return lax.dot_general(left_op, right_op, (((1,), (1,)), ((), ())), preferred_element_type=F32)


def norm_rows_of(values, gain, shift):
    wide = values.astype(F32)
    centered = wide - jnp.mean(wide, axis=-1, keepdims=True)
    variance = jnp.mean(centered * centered, axis=-1, keepdims=True)
    return (centered * lax.rsqrt(variance + EPS) * gain + shift).astype(BF16)


def gelu_tanh(v):
    k = math.sqrt(2.0 / math.pi)
    inner = v * (k + (k * 0.044715) * (v * v))
    half = 0.5 * v
    return half + half * jnp.tanh(inner)


def kernel(
    dims,
    x_ref, hint_ref, in_norm, out_norm, hint_proj, final_norm, w_out,
    in_qkv, in_proj, in_up, in_down, out_qkv, out_proj, out_up, out_down, zero_proj, skip_proj,
    y_ref,
    res, store, inbox, kk, vv, qbuf, abuf, hbuf, s_buf, p_buf, l_buf, tbuf, normf,
    wqkv, wproj, wup, wdown, wskip, zbuf, c0buf, ysend, yrecv,
    wsem, zsem, first_send, first_recv, kv_send, kv_recv, ctrl_send, box_recv, y_send, y_recv,
):
    group, n, slab, width, head_dim = dims
    n_in = n + 1
    slots = group // 2
    rows = slots * slab
    half = group // 2
    qc = rows // 2
    pair_w = 2 * head_dim
    pairs = width // pair_w
    scale = math.log2(math.e) * head_dim ** -0.5

    me = lax.axis_index("group")
    core = me % 2
    slot_me = me // 2
    base_dev = core
    ctrl_dev = half + core
    partner = me + 1 - 2 * core
    is_base = me < 2
    is_ctrl = (me >= half) & (me < half + 2)
    helper_of = 2 + 5 * core
    is_help = (me == 2) | (me == 7)
    help_core = (me == 7).astype(jnp.int32)
    branch = (me // half)

    def rcopy(src, dst, send, recv, dev):
        return pltpu.make_async_remote_copy(
            src_ref=src, dst_ref=dst, send_sem=send, recv_sem=recv, device_id={"group": dev}, device_id_type=MESH)

    barrier = pltpu.get_barrier_semaphore()
    for d in range(1, group):
        pl.semaphore_signal(barrier, inc=1, device_id={"group": (me + d) % group}, device_id_type=MESH)
    pl.semaphore_wait(barrier, group - 1)

    def w_copies(src5, idx, slot):
        out = []
        for k, (s, d) in enumerate(zip(src5, (wqkv, wproj, wup, wdown))):
            out.append(pltpu.make_async_copy(s.at[idx], d.at[slot], wsem.at[slot, k]))
        return out

    ins = (in_qkv, in_proj, in_up, in_down)
    outs = (out_qkv, out_proj, out_up, out_down)

    @pl.when(is_base | is_ctrl)
    def _():
        for c in w_copies(ins, (branch, 0), 0):
            c.start()

    slab_rows = pl.ds(pl.multiple_of(slot_me * slab, slab), slab)
    to_base = rcopy(x_ref, res.at[slab_rows], first_send.at[0], first_recv.at[slot_me], base_dev)

    @pl.when(jnp.logical_not(is_base))
    def _():
        to_base.start()

    c0buf[...] = (x_ref[...].astype(F32) + mat_f32(hint_ref[...], hint_proj[...])).astype(BF16)
    to_ctrl = rcopy(c0buf, res.at[slab_rows], first_send.at[1], first_recv.at[slot_me], ctrl_dev)

    @pl.when(jnp.logical_not(is_ctrl))
    def _():
        to_ctrl.start()

    @pl.when(is_base)
    def _():
        res[slab_rows, :] = x_ref[...]

    @pl.when(is_ctrl)
    def _():
        res[slab_rows, :] = c0buf[...]

    @pl.when(is_base | is_ctrl)
    def _():
        for s in range(slots):
            @pl.when(s != slot_me)
            def _():
                blk = res.at[pl.ds(s * slab, slab)]
                rcopy(blk, blk, first_send.at[0], first_recv.at[s], me).wait_recv()

    def block(i):
        slot = i % 2

        @pl.when(i < n_in)
        def _():
            normf[:4, :width] = in_norm[branch, jnp.minimum(i, n_in - 1)].astype(F32)

        @pl.when(i >= n_in)
        def _():
            normf[:4, :width] = out_norm[jnp.maximum(i - n_in, 0)].astype(F32)

        g1, b1, g2, b2 = (normf[k:k + 1, :width] for k in range(4))
        cps = w_copies(ins, (0, 0), slot)
        for cp in cps:
            cp.wait()
        t = norm_rows_of(res[...], g1, b1)
        sends = []
        for k, buf in enumerate((kk, vv)):
            buf[slot, 0] = mat_f32(t, wqkv[slot, :, (k + 1) * width:(k + 2) * width]).astype(BF16)
            cp = rcopy(buf.at[slot, 0], buf.at[slot, 1], kv_send.at[slot, k], kv_recv.at[slot, k], partner)
            cp.start()
            sends.append(cp)
        q = mat_f32(t, wqkv[slot, :, :width]).astype(BF16)
        low = lax.broadcasted_iota(jnp.int32, (rows, width), 1) % pair_w < head_dim
        qbuf[0] = jnp.where(low, q, jnp.zeros_like(q))
        qbuf[1] = jnp.where(low, jnp.zeros_like(q), q)

        units = [(c, p) for c in range(2) for p in range(pairs)]
        step = STEP

        low_q = lax.broadcasted_iota(jnp.int32, (qc, pair_w), 1) < head_dim

        def scores(part, u):
            c, p = units[u]
            cols = slice(p * pair_w, (p + 1) * pair_w)
            both = jnp.concatenate([qbuf[0, c * qc:(c + 1) * qc, cols], qbuf[1, c * qc:(c + 1) * qc, cols]], axis=0)
            s_buf[u, :, part * rows:(part + 1) * rows] = mat_nt(both, kk[slot, part, :, cols])

        def soften(u):
            b = u % 2
            for rb in range(0, 2 * qc, step):
                rr = slice(rb, rb + step)
                s = s_buf[u, rr, :]
                m = jnp.max(s, axis=-1, keepdims=True)
                e = jnp.exp2((s - m) * scale)
                p_buf[b, rr, :] = e.astype(BF16)
                l_buf[b, rr, :] = 1.0 / jnp.broadcast_to(jnp.sum(e, axis=-1, keepdims=True), (step, pair_w))

        def weigh(u):
            c, p = units[u]
            b = u % 2
            cols = slice(p * pair_w, (p + 1) * pair_w)
            o = (mat_f32(p_buf[b, :, :rows], vv[slot, 0, :, cols]) + mat_f32(p_buf[b, :, rows:], vv[slot, 1, :, cols])) * l_buf[b]
            abuf[c * qc:(c + 1) * qc, cols] = jnp.where(low_q, o[:qc], o[qc:]).astype(BF16)

        def mid(c):
            r = slice(c * qc, (c + 1) * qc)
            add = mat_f32(abuf[r, :], wproj[slot])
            u = (res[r, :].astype(F32) + add).astype(BF16)
            res[r, :] = u
            tbuf[r, :] = norm_rows_of(u, g2, b2)

        def up(c):
            r = slice(c * qc, (c + 1) * qc)
            hbuf[r, :] = gelu_tanh(mat_f32(tbuf[r, :], wup[slot])).astype(BF16)

        def down(c):
            r = slice(c * qc, (c + 1) * qc)
            res[r, :] = (res[r, :].astype(F32) + mat_f32(hbuf[r, :], wdown[slot])).astype(BF16)

        for u in range(len(units)):
            scores(0, u)
        sends[0].wait_recv()
        scores(1, 0)
        for u in range(len(units)):
            if u + 1 < len(units):
                scores(1, u + 1)
            if u == FILL:
                mid(0)
            if u == FILL + 1:
                up(0)
            soften(u)
            if u == 0:
                sends[1].wait_recv()
            weigh(u)
        for k in range(len(units), FILL + 2):
            (mid if k == FILL else up)(0)
        down(0)
        mid(1)
        up(1)
        down(1)
        for cp in sends:
            cp.wait_send()

    n_iter = jnp.where(is_base, n_in + n, n_in)

    def c_send(i, k):
        rr = pl.ds(k * slab, slab)
        return rcopy(store.at[i, rr], inbox.at[i, rr], ctrl_send.at[i, k], box_recv.at[i, k], helper_of)

    def box_wait(i, k):
        blk = inbox.at[i, pl.ds(k * slab, slab)]
        rcopy(blk, blk, ctrl_send.at[i, k], box_recv.at[i, k], me).wait_recv()

    def layer(i, carry):
        nxt = i + 1

        @pl.when(nxt < n_in)
        def _():
            for c in w_copies(ins, (branch, jnp.minimum(nxt, n_in - 1)), nxt % 2):
                c.start()

        @pl.when((nxt >= n_in) & (nxt < n_iter))
        def _():
            j = jnp.clip(nxt - n_in, 0, n - 1)
            for c in w_copies(outs, j, nxt % 2):
                c.start()
            pltpu.make_async_copy(skip_proj.at[j], wskip.at[nxt % 2], wsem.at[nxt % 2, 4]).start()

        @pl.when(i == n_in)
        def _():
            for k in range(slots):
                box_wait(n, k)
            res[...] = (res[...].astype(F32) + inbox[n].astype(F32)).astype(BF16)

        @pl.when(i >= n_in)
        def _():
            src = jnp.clip(n - 1 - (i - n_in), 0, n - 1)
            for k in range(slots):
                box_wait(src, k)
            slot = i % 2
            pltpu.make_async_copy(skip_proj.at[0], wskip.at[slot], wsem.at[slot, 4]).wait()
            for c in range(2):
                r = slice(c * qc, (c + 1) * qc)
                sk = (store[src, r, :].astype(F32) + inbox[src, r, :].astype(F32)).astype(BF16)
                top = mat_f32(res[r, :], wskip[slot, :width, :])
                res[r, :] = (top + mat_f32(sk, wskip[slot, width:, :])).astype(BF16)

        block(i)

        @pl.when(i < n_in)
        def _():
            ii = jnp.minimum(i, n)
            store[ii] = res[...]

            @pl.when(is_ctrl)
            def _():
                for k in range(slots):
                    c_send(ii, k).start()

        return carry

    @pl.when(is_base | is_ctrl)
    def _():
        lax.fori_loop(0, n_iter, layer, 0)

    @pl.when(is_ctrl)
    def _():
        def drain(i, a):
            for k in range(slots):
                c_send(i, k).wait_send()
            return a

        lax.fori_loop(0, n_in, drain, 0)

    @pl.when(is_help)
    def _():
        def z_copy(i):
            return pltpu.make_async_copy(zero_proj.at[i], zbuf.at[i % 2], zsem.at[i % 2])

        def r_send(i, k):
            rr = pl.ds(k * slab, slab)
            return rcopy(store.at[i, rr], inbox.at[i, rr], ctrl_send.at[i, k], box_recv.at[i, k], help_core)

        z_copy(0).start()

        def relay(i, a):
            @pl.when(i + 1 < n_in)
            def _():
                z_copy(jnp.minimum(i + 1, n)).start()

            z_copy(i).wait()
            for k in range(slots):
                r = slice(k * slab, (k + 1) * slab)
                box_wait(i, k)
                store[i, r, :] = mat_f32(inbox[i, r, :], zbuf[i % 2]).astype(BF16)
                r_send(i, k).start()
            return a

        lax.fori_loop(0, n_in, relay, 0)

        def drain(i, a):
            for k in range(slots):
                r_send(i, k).wait_send()
            return a

        lax.fori_loop(0, n_in, drain, 0)

    @pl.when(is_base)
    def _():
        gf, bf = final_norm[0:1, :].astype(F32), final_norm[1:2, :].astype(F32)
        copies = []
        for s in range(slots):
            t = norm_rows_of(res[s * slab:(s + 1) * slab, :], gf, bf)
            y = mat_f32(t, w_out[...]).astype(BF16)
            if s == 0:
                y_ref[...] = y
            else:
                ysend[s] = y
                cp = rcopy(ysend.at[s], yrecv, y_send.at[s], y_recv, 2 * s + core)
                cp.start()
                copies.append(cp)
        for cp in copies:
            cp.wait_send()

    @pl.when(jnp.logical_not(is_base))
    def _():
        to_base.wait_send()
        rcopy(yrecv, yrecv, y_send.at[0], y_recv, me).wait_recv()
        y_ref[...] = yrecv[...]

    @pl.when(jnp.logical_not(is_ctrl))
    def _():
        to_ctrl.wait_send()


def solution(mesh):
    group = mesh.shape["group"]

    def device_step(x_own, hint_own, in_qkv, in_proj, in_up, in_down, in_norm, out_qkv, out_proj, out_up, out_down, out_norm, zero_proj, hint_proj, skip_proj, final_norm, w_out):
        slab, width = x_own.shape
        n = skip_proj.shape[0]
        heads, head_dim = in_proj.shape[2], in_proj.shape[3]
        hidden = in_up.shape[-1]
        rows = (group // 2) * slab
        qc = rows // 2
        in_proj = in_proj.reshape(in_proj.shape[:2] + (width, width))
        out_proj = out_proj.reshape(out_proj.shape[:1] + (width, width))
        vm = pl.BlockSpec(memory_space=pltpu.VMEM)
        hb = pl.BlockSpec(memory_space=pl.ANY)
        dma = pltpu.SemaphoreType.DMA
        return pl.pallas_call(
            functools.partial(kernel, (group, n, slab, width, head_dim)),
            out_shape=jax.ShapeDtypeStruct((slab, width), BF16),
            in_specs=[vm] * 7 + [hb] * 10,
            out_specs=vm,
            scratch_shapes=[
                pltpu.VMEM((rows, width), BF16),
                pltpu.VMEM((n + 1, rows, width), BF16),
                pltpu.VMEM((n + 1, rows, width), BF16),
                pltpu.VMEM((2, 2, rows, width), BF16),
                pltpu.VMEM((2, 2, rows, width), BF16),
                pltpu.VMEM((2, rows, width), BF16),
                pltpu.VMEM((rows, width), BF16),
                pltpu.VMEM((rows, hidden), BF16),
                pltpu.VMEM((heads, 2 * qc, 2 * rows), F32),
                pltpu.VMEM((2, 2 * qc, 2 * rows), BF16),
                pltpu.VMEM((2, 2 * qc, 2 * head_dim), F32),
                pltpu.VMEM((rows, width), BF16),
                pltpu.VMEM((8, 2 * qc), F32),
                pltpu.VMEM((2, width, 3 * width), BF16),
                pltpu.VMEM((2, width, width), BF16),
                pltpu.VMEM((2, width, hidden), BF16),
                pltpu.VMEM((2, hidden, width), BF16),
                pltpu.VMEM((2, 2 * width, width), BF16),
                pltpu.VMEM((2, width, width), BF16),
                pltpu.VMEM((slab, width), BF16),
                pltpu.VMEM((group // 2, slab, width), BF16),
                pltpu.VMEM((slab, width), BF16),
                dma((2, 5)), dma((2,)),
                dma((2,)), dma((group // 2,)),
                dma((2, 2)), dma((2, 2)),
                dma((n + 1, group // 2)), dma((n + 1, group // 2)),
                dma((group // 2,)), dma,
            ],
            compiler_params=pltpu.CompilerParams(
                collective_id=0, has_side_effects=True, vmem_limit_bytes=60 * 1024 * 1024, internal_scratch_in_bytes=5 * 16384),
        )(x_own, hint_own, in_norm, out_norm, hint_proj, final_norm, w_out,
          in_qkv, in_proj, in_up, in_down, out_qkv, out_proj, out_up, out_down, zero_proj, skip_proj)

    tok_spec = P(("data", "group"), None)
    return jax.shard_map(device_step, mesh=mesh, in_specs=(tok_spec, tok_spec) + (P(),) * 15, out_specs=tok_spec, check_vma=False)
```

```python
import functools
import math

import jax
import jax.numpy as jnp
from jax import lax
from jax.experimental import pallas as pl
from jax.experimental.pallas import tpu as pltpu
from jax.sharding import PartitionSpec as P

EPS = 1e-6
FILL = 9
WAIT_K, WAIT_V = 5, 6
MESH = pl.DeviceIdType.MESH
F32, BF16 = jnp.float32, jnp.bfloat16


def mat_f32(left_op, right_op):
    return jnp.dot(left_op, right_op, preferred_element_type=F32)


def mat_nt(left_op, right_op):
    return lax.dot_general(left_op, right_op, (((1,), (1,)), ((), ())), preferred_element_type=F32)


def norm_rows_of(values, gain, shift):
    wide = values.astype(F32)
    centered = wide - jnp.mean(wide, axis=-1, keepdims=True)
    variance = jnp.mean(centered * centered, axis=-1, keepdims=True)
    return (centered * lax.rsqrt(variance + EPS) * gain + shift).astype(BF16)


def gelu_tanh(v):
    k = math.sqrt(2.0 / math.pi)
    inner = v * (k + (k * 0.044715) * (v * v))
    half = 0.5 * v
    return half + half * jnp.tanh(inner)


def kernel(
    dims,
    x_ref, hint_ref, in_norm, out_norm, hint_proj, final_norm, w_out,
    in_qkv, in_proj, in_up, in_down, out_qkv, out_proj, out_up, out_down, zero_proj, skip_proj,
    y_ref,
    res, store, inbox, kk, vt, qbuf, abuf, hbuf, s_buf, p_buf, obuf, ml_buf, tbuf, normf,
    wqkv, wproj, wup, wdown, wskip, wlow, low_part, zbuf, c0buf, ysend, yrecv,
    wsem, lsem, zsem, first_send, first_recv, kv_send, kv_recv, ctrl_send, box_recv, y_send, y_recv,
):
    group, n, slab, width, head_dim = dims
    n_in = n + 1
    slots = group // 2
    rows = slots * slab
    half = group // 2
    qc = rows // 2
    pair_w = 2 * head_dim
    pairs = width // pair_w
    scale = math.log2(math.e) * head_dim ** -0.5

    me = lax.axis_index("group")
    core = me % 2
    slot_me = me // 2
    base_dev = core
    ctrl_dev = half + core
    partner = me + 1 - 2 * core
    is_base = me < 2
    is_ctrl = (me >= half) & (me < half + 2)
    helper_of = 2 + 5 * core
    is_help = (me == 2) | (me == 7)
    help_core = (me == 7).astype(jnp.int32)
    branch = (me // half)

    def rcopy(src, dst, send, recv, dev):
        return pltpu.make_async_remote_copy(
            src_ref=src, dst_ref=dst, send_sem=send, recv_sem=recv, device_id={"group": dev}, device_id_type=MESH)

    barrier = pltpu.get_barrier_semaphore()
    for d in range(1, group):
        pl.semaphore_signal(barrier, inc=1, device_id={"group": (me + d) % group}, device_id_type=MESH)
    pl.semaphore_wait(barrier, group - 1)

    def w_copies(src5, idx, slot):
        out = []
        for k, (s, d) in enumerate(zip(src5, (wqkv, wproj, wup, wdown))):
            out.append(pltpu.make_async_copy(s.at[idx], d.at[slot], wsem.at[slot, k]))
        return out

    def top_copy(j, slot):
        return pltpu.make_async_copy(skip_proj.at[j, pl.ds(0, width)], wskip.at[slot], wsem.at[slot, 4])

    def low_copy(a):
        return pltpu.make_async_copy(skip_proj.at[n - 1 - a, pl.ds(width, width)], wlow.at[a], lsem.at[a])

    ins = (in_qkv, in_proj, in_up, in_down)
    outs = (out_qkv, out_proj, out_up, out_down)

    @pl.when(is_base | is_ctrl)
    def _():
        for c in w_copies(ins, (branch, 0), 0):
            c.start()

    slab_rows = pl.ds(pl.multiple_of(slot_me * slab, slab), slab)
    to_base = rcopy(x_ref, res.at[slab_rows], first_send.at[0], first_recv.at[slot_me], base_dev)
    c0buf[...] = (x_ref[...].astype(F32) + mat_f32(hint_ref[...], hint_proj[...])).astype(BF16)
    to_ctrl = rcopy(c0buf, res.at[slab_rows], first_send.at[1], first_recv.at[slot_me], ctrl_dev)

    @pl.when(jnp.logical_not(is_ctrl))
    def _():
        to_ctrl.start()

    @pl.when(jnp.logical_not(is_base))
    def _():
        to_base.start()

    @pl.when(is_base)
    def _():
        res[slab_rows, :] = x_ref[...]

    @pl.when(is_ctrl)
    def _():
        res[slab_rows, :] = c0buf[...]

    @pl.when(is_base | is_ctrl)
    def _():
        for s in range(slots):
            @pl.when(s != slot_me)
            def _():
                blk = res.at[pl.ds(s * slab, slab)]
                rcopy(blk, blk, first_send.at[0], first_recv.at[s], me).wait_recv()

    def block(i):
        slot = i % 2

        @pl.when(i < n_in)
        def _():
            normf[:4, :width] = in_norm[branch, jnp.minimum(i, n_in - 1)].astype(F32)

        @pl.when(i >= n_in)
        def _():
            normf[:4, :width] = out_norm[jnp.maximum(i - n_in, 0)].astype(F32)

        g1, b1, g2, b2 = (normf[k:k + 1, :width] for k in range(4))
        cps = w_copies(ins, (0, 0), slot)
        for cp in cps:
            cp.wait()
        t = norm_rows_of(res[...], g1, b1)
        kk[slot, 0] = mat_f32(t, wqkv[slot, :, width:2 * width]).astype(BF16)
        vt[slot, 0] = lax.dot_general(wqkv[slot, :, 2 * width:], t, (((0,), (1,)), ((), ())), preferred_element_type=F32).astype(BF16)
        sends = []
        for k, buf in enumerate((kk, vt)):
            cp = rcopy(buf.at[slot, 0], buf.at[slot, 1], kv_send.at[slot, k], kv_recv.at[slot, k], partner)
            cp.start()
            sends.append(cp)
        q = mat_f32(t, wqkv[slot, :, :width]).astype(BF16)
        low = lax.broadcasted_iota(jnp.int32, (rows, width), 1) % pair_w < head_dim
        qbuf[0] = jnp.where(low, q, jnp.zeros_like(q))
        qbuf[1] = jnp.where(low, jnp.zeros_like(q), q)

        units = [(c, p) for c in range(2) for p in range(pairs)]
        step = 256

        def scores(part, u):
            c, p = units[u]
            cols = slice(p * pair_w, (p + 1) * pair_w)
            both = jnp.concatenate([qbuf[0, c * qc:(c + 1) * qc, cols], qbuf[1, c * qc:(c + 1) * qc, cols]], axis=0)
            s_buf[u % 2] = mat_nt(kk[slot, part, :, cols], both)

        def fold(v, op):
            return op(v.reshape(-1, 8, v.shape[-1]), axis=0)

        def peak(part, u):
            b = u % 2
            m8 = fold(s_buf[b, 0:step, :], jnp.max)
            for rb in range(step, rows, step):
                m8 = jnp.maximum(m8, fold(s_buf[b, rb:rb + step, :], jnp.max))
            return jnp.max(m8, axis=0, keepdims=True)

        def soften(part, u, m):
            b = u % 2
            st = 2 * u
            fix = None
            if part == 1:
                m_old = ml_buf[st:st + 1, :]
                m = jnp.maximum(m, m_old)
                fix = jnp.exp2((m_old - m) * scale)
            m8 = jnp.broadcast_to(m, (8, 2 * qc))
            l8 = jnp.zeros_like(m8)
            for rb in range(0, rows, step):
                s3 = s_buf[b, rb:rb + step, :].reshape(step // 8, 8, 2 * qc)
                e = jnp.exp2((s3 - m8[None]) * scale)
                p_buf[b, rb:rb + step, :] = e.reshape(step, 2 * qc).astype(BF16)
                l8 = l8 + jnp.sum(e, axis=0)
                m8 = jnp.where(l8 >= 0.0, m8, l8)
            l = jnp.sum(l8, axis=0, keepdims=True)
            if part == 0:
                ml_buf[st:st + 1, :] = m
                ml_buf[st + 1:st + 2, :] = l
                return None, None
            return fix, 1.0 / (l + ml_buf[st + 1:st + 2, :] * fix)

        def weigh(part, u, fix, inv):
            c, p = units[u]
            b = u % 2
            r = slice(c * qc, (c + 1) * qc)
            for hh in range(2):
                lanes = slice(hh * qc, (hh + 1) * qc)
                h = 2 * p + hh
                hr = slice(h * head_dim, (h + 1) * head_dim)
                o = mat_f32(vt[slot, part, hr, :], p_buf[b, :, lanes])
                if part == 0:
                    obuf[hr, r] = o
                else:
                    abuf[hr, r] = ((o + obuf[hr, r] * fix[:, lanes]) * inv[:, lanes]).astype(BF16)

        def mid(c):
            r = slice(c * qc, (c + 1) * qc)
            add = lax.dot_general(abuf[:, r], wproj[slot], (((0,), (0,)), ((), ())), preferred_element_type=F32)
            u = (res[r, :].astype(F32) + add).astype(BF16)
            res[r, :] = u
            tbuf[r, :] = norm_rows_of(u, g2, b2)

        def up(c):
            r = slice(c * qc, (c + 1) * qc)
            hbuf[r, :] = gelu_tanh(mat_f32(tbuf[r, :], wup[slot])).astype(BF16)

        def down(c):
            r = slice(c * qc, (c + 1) * qc)
            res[r, :] = (res[r, :].astype(F32) + mat_f32(hbuf[r, :], wdown[slot])).astype(BF16)

        order = [(part, u) for part in range(2) for u in range(len(units))]
        scores(*order[0])
        m_next = peak(*order[0])
        for k, (part, u) in enumerate(order):
            if k == WAIT_K:
                sends[0].wait_recv()
            if k == WAIT_V:
                sends[1].wait_recv()
            m = m_next
            if k + 1 < len(order):
                scores(*order[k + 1])
                m_next = peak(*order[k + 1])
            if k == FILL:
                mid(0)
            if k == FILL + 1:
                up(0)
            weigh(part, u, *soften(part, u, m))
        for k in range(len(order), FILL + 2):
            (mid if k == FILL else up)(0)
        down(0)
        mid(1)
        up(1)
        down(1)
        for cp in sends:
            cp.wait_send()

    n_iter = jnp.where(is_base, n_in + n, n_in)

    def c_send(i, k):
        rr = pl.ds(k * slab, slab)
        return rcopy(store.at[i, rr], inbox.at[i, rr], ctrl_send.at[i, k], box_recv.at[i, k], helper_of)

    def box_wait(i, k):
        blk = inbox.at[i, pl.ds(k * slab, slab)]
        rcopy(blk, blk, ctrl_send.at[i, k], box_recv.at[i, k], me).wait_recv()

    def layer(i, carry):
        nxt = i + 1

        @pl.when(nxt < n_in)
        def _():
            for c in w_copies(ins, (branch, jnp.minimum(nxt, n_in - 1)), nxt % 2):
                c.start()

        @pl.when((nxt >= n_in) & (nxt < n_iter))
        def _():
            j = jnp.clip(nxt - n_in, 0, n - 1)
            for c in w_copies(outs, j, nxt % 2):
                c.start()
            top_copy(j, nxt % 2).start()

        @pl.when((i == n) & is_base)
        def _():
            def fetch(a, z):
                low_copy(a).start()
                return z

            lax.fori_loop(0, n, fetch, 0)

        @pl.when(i == n_in)
        def _():
            def skip_low(a, z):
                for k in range(slots):
                    box_wait(a, k)
                low_copy(a).wait()
                sk = (store[a].astype(F32) + inbox[a].astype(F32)).astype(BF16)
                low_part[a] = mat_f32(sk, wlow[a])
                return z

            lax.fori_loop(0, n, skip_low, 0)
            for k in range(slots):
                box_wait(n, k)
            res[...] = (res[...].astype(F32) + inbox[n].astype(F32)).astype(BF16)

        @pl.when(i >= n_in)
        def _():
            src = jnp.clip(n - 1 - (i - n_in), 0, n - 1)
            top_copy(0, i % 2).wait()
            res[...] = (mat_f32(res[...], wskip[i % 2]) + low_part[src]).astype(BF16)

        block(i)

        @pl.when(i < n_in)
        def _():
            ii = jnp.minimum(i, n)
            store[ii] = res[...]

            @pl.when(is_ctrl)
            def _():
                for k in range(slots):
                    c_send(ii, k).start()

        return carry

    @pl.when(is_base | is_ctrl)
    def _():
        lax.fori_loop(0, n_iter, layer, 0)

    @pl.when(is_ctrl)
    def _():
        def drain(i, a):
            for k in range(slots):
                c_send(i, k).wait_send()
            return a

        lax.fori_loop(0, n_in, drain, 0)

    @pl.when(is_help)
    def _():
        def z_copy(i):
            return pltpu.make_async_copy(zero_proj.at[i], zbuf.at[i % 2], zsem.at[i % 2])

        def r_send(i, k):
            rr = pl.ds(k * slab, slab)
            return rcopy(store.at[i, rr], inbox.at[i, rr], ctrl_send.at[i, k], box_recv.at[i, k], help_core)

        z_copy(0).start()

        def relay(i, a):
            @pl.when(i + 1 < n_in)
            def _():
                z_copy(jnp.minimum(i + 1, n)).start()

            z_copy(i).wait()
            for k in range(slots):
                r = slice(k * slab, (k + 1) * slab)
                box_wait(i, k)
                store[i, r, :] = mat_f32(inbox[i, r, :], zbuf[i % 2]).astype(BF16)
                r_send(i, k).start()
            return a

        lax.fori_loop(0, n_in, relay, 0)

        def drain(i, a):
            for k in range(slots):
                r_send(i, k).wait_send()
            return a

        lax.fori_loop(0, n_in, drain, 0)

    @pl.when(is_base)
    def _():
        gf, bf = final_norm[0:1, :].astype(F32), final_norm[1:2, :].astype(F32)
        copies = []
        for s in [slots // 2] + [k for k in range(1, slots) if k != slots // 2] + [0]:
            t = norm_rows_of(res[s * slab:(s + 1) * slab, :], gf, bf)
            y = mat_f32(t, w_out[...]).astype(BF16)
            if s == 0:
                y_ref[...] = y
            else:
                ysend[s] = y
                cp = rcopy(ysend.at[s], yrecv, y_send.at[s], y_recv, 2 * s + core)
                cp.start()
                copies.append(cp)
        for cp in copies:
            cp.wait_send()

    @pl.when(jnp.logical_not(is_base))
    def _():
        to_base.wait_send()
        rcopy(yrecv, yrecv, y_send.at[0], y_recv, me).wait_recv()
        y_ref[...] = yrecv[...]

    @pl.when(jnp.logical_not(is_ctrl))
    def _():
        to_ctrl.wait_send()


def solution(mesh):
    group = mesh.shape["group"]

    def device_step(x_own, hint_own, in_qkv, in_proj, in_up, in_down, in_norm, out_qkv, out_proj, out_up, out_down, out_norm, zero_proj, hint_proj, skip_proj, final_norm, w_out):
        slab, width = x_own.shape
        n = skip_proj.shape[0]
        heads, head_dim = in_proj.shape[2], in_proj.shape[3]
        hidden = in_up.shape[-1]
        rows = (group // 2) * slab
        qc = rows // 2
        in_proj = in_proj.reshape(in_proj.shape[:2] + (width, width))
        out_proj = out_proj.reshape(out_proj.shape[:1] + (width, width))
        vm = pl.BlockSpec(memory_space=pltpu.VMEM)
        hb = pl.BlockSpec(memory_space=pl.ANY)
        dma = pltpu.SemaphoreType.DMA
        return pl.pallas_call(
            functools.partial(kernel, (group, n, slab, width, head_dim)),
            out_shape=jax.ShapeDtypeStruct((slab, width), BF16),
            in_specs=[vm] * 7 + [hb] * 10,
            out_specs=vm,
            scratch_shapes=[
                pltpu.VMEM((rows, width), BF16),
                pltpu.VMEM((n + 1, rows, width), BF16),
                pltpu.VMEM((n + 1, rows, width), BF16),
                pltpu.VMEM((2, 2, rows, width), BF16),
                pltpu.VMEM((2, 2, width, rows), BF16),
                pltpu.VMEM((2, rows, width), BF16),
                pltpu.VMEM((width, rows), BF16),
                pltpu.VMEM((rows, hidden), BF16),
                pltpu.VMEM((2, rows, 2 * qc), F32),
                pltpu.VMEM((2, rows, 2 * qc), BF16),
                pltpu.VMEM((width, rows), F32),
                pltpu.VMEM((2 * heads, 2 * qc), F32),
                pltpu.VMEM((rows, width), BF16),
                pltpu.VMEM((8, 2 * qc), F32),
                pltpu.VMEM((2, width, 3 * width), BF16),
                pltpu.VMEM((2, width, width), BF16),
                pltpu.VMEM((2, width, hidden), BF16),
                pltpu.VMEM((2, hidden, width), BF16),
                pltpu.VMEM((2, width, width), BF16),
                pltpu.VMEM((n, width, width), BF16),
                pltpu.VMEM((n, rows, width), F32),
                pltpu.VMEM((2, width, width), BF16),
                pltpu.VMEM((slab, width), BF16),
                pltpu.VMEM((group // 2, slab, width), BF16),
                pltpu.VMEM((slab, width), BF16),
                dma((2, 5)), dma((n,)), dma((2,)),
                dma((2,)), dma((group // 2,)),
                dma((2, 2)), dma((2, 2)),
                dma((n + 1, group // 2)), dma((n + 1, group // 2)),
                dma((group // 2,)), dma,
            ],
            compiler_params=pltpu.CompilerParams(
                collective_id=0, has_side_effects=True, vmem_limit_bytes=60 * 1024 * 1024, internal_scratch_in_bytes=5 * 16384),
        )(x_own, hint_own, in_norm, out_norm, hint_proj, final_norm, w_out,
          in_qkv, in_proj, in_up, in_down, out_qkv, out_proj, out_up, out_down, zero_proj, skip_proj)

    tok_spec = P(("data", "group"), None)
    return jax.shard_map(device_step, mesh=mesh, in_specs=(tok_spec, tok_spec) + (P(),) * 15, out_specs=tok_spec, check_vma=False)
```
